128 devices in a mesh: zero: 16 (over z, y), width: 8 (over x, core).
Axes of the slice: x: 4, y: 4, z: 4, core: 2. Of those that a mesh axis runs over, the one named last changes fastest.
Arguments:
- train_query: float32 [7168, 7168], P('zero', 'width'), may hold values from -0.09375 to 0.09375
- slow_query: float32 [7168, 7168], P('zero', 'width'), may hold values from -0.0625 to 0.0625
- train_key: float32 [7168, 1024], P('zero', 'width'), may hold values from -0.09375 to 0.09375
- slow_key: float32 [7168, 1024], P('zero', 'width'), may hold values from -0.0625 to 0.0625
- train_value: float32 [7168, 1024], P('zero', 'width'), may hold values from -0.09375 to 0.09375
- slow_value: float32 [7168, 1024], P('zero', 'width'), may hold values from -0.0625 to 0.0625
- norm_train: float32 [7168], P(('zero', 'width')), may hold values from 0.25 to 1.75
- norm_step: float32 [7168], P(('zero', 'width')), may hold values from -0.3 to 0.3
Outputs:
- ready_query: bfloat16 [7168, 7168], P(None, 'width')
- ready_key: bfloat16 [7168, 1024], P(None, 'width')
- ready_value: bfloat16 [7168, 1024], P(None, 'width')
- scale_query: float32 [7168], P('width')
- scale_key: float32 [1024], P('width')
- scale_value: float32 [1024], P('width')
- serve_norm: bfloat16 [7168], replicated
- latest_query: float32 [7168, 7168], P('zero', 'width')
- latest_key: float32 [7168, 1024], P('zero', 'width')
- latest_value: float32 [7168, 1024], P('zero', 'width')
The draws below stay inside these ranges and needn't reach their ends.
All inputs are finite; a program needn't handle non-finite values.
Results may differ from the reference program's by a relative error of at most 0.0004.
Values may be sent and summed in bfloat16 or wider, within the bound.
A program may use at most 128 MiB of HBM per device.

```python
import jax
import jax.numpy as jnp
from jax import lax

D_MODEL = 7168
Q_DIM = 7168
KV_DIM = 1024


def strengthened(result, key, source, target, blocks, factor):
    def block_of(dim):
        return (jnp.arange(result.shape[dim]) // (result.shape[dim] // blocks)).reshape((-1,) + (1,) * (result.ndim - 1 - dim))

    near = jax.random.permutation(key, blocks)[block_of(target)]
    far = (block_of(target) + blocks // 2) % blocks
    return jnp.where((block_of(source) == near) | (block_of(source) == far), factor * result, result)


def levels(stream_key, extent, shards, smallest, high):
    def one(position, parts):
        heights = jax.random.uniform(jax.random.fold_in(jax.random.fold_in(stream_key, 6), position), (parts,), jnp.float32, smallest / len(shards), high / len(shards))
        return jnp.repeat(jnp.exp(heights), extent[position] // parts).reshape((-1,) + (1,) * (len(extent) - position - 1))

    factor_of = one(*shards[0])
    for cut in shards[1:]:
        factor_of = factor_of * one(*cut)
    return factor_of


def bell_draw(rng, extent, deviation, limit, shards=(), kind=jnp.bfloat16):
    entries = deviation * jax.random.normal(rng, extent, jnp.float32)
    if shards:
        entries = entries * levels(rng, extent, shards, -0.22, 0.18)
    return jnp.clip(entries, -limit, limit).astype(kind)


def noise_with(own_key, dims, deviation, bound, pieces, heavy, dtype=jnp.bfloat16):
    entries = deviation * jax.random.normal(own_key, dims, jnp.float32)
    if pieces:
        entries = entries * levels(own_key, dims, pieces, -0.22, 0.18)
    return jnp.clip(strengthened(entries, jax.random.fold_in(own_key, 3), *heavy), -bound, bound).astype(dtype)


def setup_inputs(seed: int = 0) -> dict:
    seeds = jax.random.split(jax.random.key(seed), 9)
    train_query = noise_with(seeds[0], (D_MODEL, Q_DIM), D_MODEL ** -0.5, 0.09375, ((0, 16), (1, 8)), (0, 1, 16, 2.0), jnp.float32)
    slow_query = bell_draw(seeds[1], (D_MODEL, Q_DIM), D_MODEL ** -0.5, 0.0625, ((0, 16), (1, 8)), jnp.float32)
    train_key = noise_with(seeds[2], (D_MODEL, KV_DIM), D_MODEL ** -0.5, 0.09375, ((0, 16), (1, 8)), (0, 1, 16, 2.0), jnp.float32)
    slow_key = bell_draw(seeds[3], (D_MODEL, KV_DIM), D_MODEL ** -0.5, 0.0625, ((0, 16), (1, 8)), jnp.float32)
    train_value = noise_with(seeds[4], (D_MODEL, KV_DIM), D_MODEL ** -0.5, 0.09375, ((0, 16), (1, 8)), (0, 1, 16, 2.0), jnp.float32)
    slow_value = bell_draw(seeds[5], (D_MODEL, KV_DIM), D_MODEL ** -0.5, 0.0625, ((0, 16), (1, 8)), jnp.float32)
    norm_train = jnp.clip(1.0 + 0.15 * jax.random.normal(seeds[6], (D_MODEL,), jnp.float32), 0.25, 1.75)
    norm_step = jnp.clip(jax.random.uniform(seeds[7], (D_MODEL,), jnp.float32, -0.3, 0.3) * levels(seeds[7], (D_MODEL,), ((0, 128),), -0.4, 0.0), -0.3, 0.3)
    return {"train_query": train_query, "slow_query": slow_query, "train_key": train_key, "slow_key": slow_key, "train_value": train_value, "slow_value": slow_value, "norm_train": norm_train, "norm_step": norm_step}


keep_rate = 0.5

def reference(train_query, slow_query, train_key, slow_key, train_value, slow_value, norm_train, norm_step):
    latest_query = keep_rate * slow_query + (1.0 - keep_rate) * train_query
    latest_key = keep_rate * slow_key + (1.0 - keep_rate) * train_key
    latest_value = keep_rate * slow_value + (1.0 - keep_rate) * train_value
    scale_query = jnp.sqrt(lax.optimization_barrier(jnp.sum(latest_query * latest_query, axis=0)))
    ready_query = (latest_query / scale_query).astype(jnp.bfloat16)
    scale_key = jnp.sqrt(lax.optimization_barrier(jnp.sum(latest_key * latest_key, axis=0)))
    ready_key = (latest_key / scale_key).astype(jnp.bfloat16)
    scale_value = jnp.sqrt(lax.optimization_barrier(jnp.sum(latest_value * latest_value, axis=0)))
    ready_value = (latest_value / scale_value).astype(jnp.bfloat16)
    serve_norm = (norm_train + norm_step).astype(jnp.bfloat16)
    return (ready_query, ready_key, ready_value, scale_query, scale_key, scale_value, serve_norm, latest_query, latest_key, latest_value)
```

```python
import functools

import jax
import jax.numpy as jnp
from jax import lax
from jax.experimental import pallas as pl
from jax.experimental.pallas import tpu as pltpu
from jax.sharding import PartitionSpec as P

keep_rate = 0.5
MESH = pl.DeviceIdType.MESH

NZ, NY, NW = 4, 4, 8
NZERO = NZ * NY
ROWS = 448
WQ, WK = 896, 128
COLS = WQ + 2 * WK
QUARTER = ROWS // 4
SLAB = 16
NORM = 56

ORDER = (
    ("one", 0),
    ("two", 0, 0),
    ("one", 1),
    ("two", 1, 0),
    ("one", 2),
    ("two", 2, 0),
    ("two", 0, 1),
    ("two", 3, 0),
    ("two", 1, 1),
    ("two", 2, 1),
    ("two", 0, 2),
    ("two", 3, 1),
    ("two", 1, 2),
    ("two", 2, 2),
    ("two", 3, 2),
)
SLOT = {entry: at for at, entry in enumerate(ORDER)}
LINKS = (("y", 1), ("y", -1), ("z", 1), ("z", -1))
PARTNER = (2, 3, 0, 1)


def gather_kernel(
    tq, sq, tk, sk, tv, sv, nt, ns,
    all_ref, lat_ref, cq_ref, ck_ref, cv_ref, norm_ref,
    tbuf, sbuf, sums, ntb, nsb, nbuf,
    load_sem, nload_sem, sum_send, sum_recv, na_send, na_recv, nb_send, nb_recv,
    send_sem, recv_sem,
):
    me = lax.axis_index("zero")
    wide = lax.axis_index("width")
    z, y = me // NY, me % NY

    def at(zz, yy):
        return lax.rem(zz + 2 * NZ, NZ) * NY + lax.rem(yy + 2 * NY, NY)

    barrier = pltpu.get_barrier_semaphore()
    for d in range(1, NZERO):
        pl.semaphore_signal(
            barrier, inc=1, device_id=(lax.rem(me + d, NZERO), wide), device_id_type=MESH
        )
    for d in range(1, NW):
        pl.semaphore_signal(
            barrier, inc=1, device_id=(me, lax.rem(wide + d, NW)), device_id_type=MESH
        )

    loads = []
    for c in range(4):
        rows = pl.ds(c * QUARTER, QUARTER)
        group = []
        for i, (src, buf, first, width) in enumerate((
            (tq, tbuf, 0, WQ), (sq, sbuf, 0, WQ),
            (tk, tbuf, WQ, WK), (sk, sbuf, WQ, WK),
            (tv, tbuf, WQ + WK, WK), (sv, sbuf, WQ + WK, WK),
        )):
            copy = pltpu.make_async_copy(
                src.at[rows], buf.at[rows, pl.ds(first, width)], load_sem.at[c, i]
            )
            copy.start()
            group.append(copy)
        loads.append(group)
    nload = (
        pltpu.make_async_copy(nt, ntb, nload_sem.at[0]),
        pltpu.make_async_copy(ns, nsb, nload_sem.at[1]),
    )
    for copy in nload:
        copy.start()

    acc = jnp.zeros((8, COLS), jnp.float32)
    for c in range(4):
        for copy in loads[c]:
            copy.wait()

        def average(i, acc):
            rows = pl.ds(pl.multiple_of(c * QUARTER + i * SLAB, SLAB), SLAB)
            latest = keep_rate * sbuf[rows, :] + (1.0 - keep_rate) * tbuf[rows, :]
            lat_ref[rows, :] = latest
            square = latest * latest
            return acc + square[:8] + square[8:]

        acc = lax.fori_loop(0, QUARTER // SLAB, average, acc)
    sums[me] = jnp.sum(acc, axis=0, keepdims=True)
    for copy in nload:
        copy.wait()
    mine = (ntb[...] + nsb[...]).reshape(1, NORM)
    nbuf[me, wide] = jnp.concatenate([mine, jnp.zeros((1, 128 - NORM), jnp.float32)], axis=1)

    pl.semaphore_wait(barrier, NZERO - 1 + NW - 1)

    small = []
    for d in range(1, NZERO):
        copy = pltpu.make_async_remote_copy(
            src_ref=sums.at[me], dst_ref=sums.at[me],
            send_sem=sum_send.at[d], recv_sem=sum_recv.at[d],
            device_id=(lax.rem(me + d, NZERO), wide), device_id_type=MESH,
        )
        copy.start()
        small.append(copy)
    across = []
    for d in range(1, NW):
        copy = pltpu.make_async_remote_copy(
            src_ref=nbuf.at[me, wide], dst_ref=nbuf.at[me, wide],
            send_sem=na_send.at[d], recv_sem=na_recv.at[d],
            device_id=(me, lax.rem(wide + d, NW)), device_id_type=MESH,
        )
        copy.start()
        across.append(copy)
    for copy in small:
        copy.wait()

    total = sums[0]
    for d in range(1, NZERO):
        total = total + sums[d]
    scale = jnp.sqrt(total)
    for r in range(WQ // 128):
        cq_ref[pl.ds(r, 1), :] = scale[:, r * 128 : (r + 1) * 128]
    ck_ref[...] = scale[:, WQ : WQ + WK]
    cv_ref[...] = scale[:, WQ + WK :]
    inverse = jnp.broadcast_to(1.0 / scale, (SLAB, COLS))

    copies = {}

    def piece(p, zz, yy):
        first = at(zz, yy) * ROWS + p * QUARTER
        return pl.ds(pl.multiple_of(first, QUARTER), QUARTER)

    def start(link, slot):
        ring, sign = LINKS[link]
        entry = ORDER[slot]
        if entry[0] == "one":
            p, j, k = link, 0, entry[1]
            if k > 0:
                copies[link, SLOT["one", k - 1]].wait_recv()
            steps = {ring: k}
        else:
            p, j, k = PARTNER[link], entry[1], entry[2]
            if k > 0:
                copies[link, SLOT["two", j, k - 1]].wait_recv()
            elif j == 3:
                copies[p, SLOT["one", 2]].wait_recv()
            steps = {ring: k, LINKS[p][0]: j}
        rows = piece(p, z - sign * steps.get("z", 0), y - sign * steps.get("y", 0))
        target = at(z + sign, y) if ring == "z" else at(z, y + sign)
        copy = pltpu.make_async_remote_copy(
            src_ref=all_ref.at[rows], dst_ref=all_ref.at[rows],
            send_sem=send_sem.at[link, slot], recv_sem=recv_sem.at[link, slot],
            device_id=(target, wide), device_id_type=MESH,
        )
        copy.start()
        copies[link, slot] = copy

    for p in range(4):
        def narrow(i, _):
            rows = pl.ds(pl.multiple_of(p * QUARTER + i * SLAB, SLAB), SLAB)
            there = pl.ds(pl.multiple_of(me * ROWS + p * QUARTER + i * SLAB, SLAB), SLAB)
            all_ref[there, :] = (lat_ref[rows, :] * inverse).astype(jnp.bfloat16)
            return 0

        lax.fori_loop(0, QUARTER // SLAB, narrow, 0)
        start(p, 0)
    for link in range(4):
        start(link, 1)

    for copy in across:
        copy.wait()
    on = []
    for d in range(1, NZERO):
        copy = pltpu.make_async_remote_copy(
            src_ref=nbuf.at[me], dst_ref=nbuf.at[me],
            send_sem=nb_send.at[d], recv_sem=nb_recv.at[d],
            device_id=(lax.rem(me + d, NZERO), wide), device_id_type=MESH,
        )
        copy.start()
        on.append(copy)

    for slot in range(2, 6):
        for link in range(4):
            start(link, slot)

    for copy in on:
        copy.wait()
    lane = lax.broadcasted_iota(jnp.int32, (1, 128), 1)
    for r in range(NZERO * NW * NORM // 128):
        row = jnp.zeros((1, 128), jnp.float32)
        for d in range(128 * r // NORM, (128 * r + 127) // NORM + 1):
            shift = d * NORM - 128 * r
            moved = pltpu.roll(nbuf[d // NW, d % NW], shift % 128, 1)
            row = jnp.where((lane >= shift) & (lane < shift + NORM), moved, row)
        norm_ref[pl.ds(r, 1), :] = row

    for slot in range(6, len(ORDER)):
        for link in range(4):
            start(link, slot)

    for slot in range(len(ORDER)):
        for link in range(4):
            copies[link, slot].wait_send()
    waited = {("one", 0), ("one", 1), ("one", 2)}
    waited |= {("two", j, k) for j in range(4) for k in range(2)}
    for entry in ORDER:
        if entry not in waited:
            for link in range(4):
                copies[link, SLOT[entry]].wait_recv()


def write_kernel(
    all_ref, lat_ref, sq_ref, sk_ref, sv_ref, norm_ref,
    rq, rk, rv, cq, ck, cv, norm_out, lq, lk, lv,
    norm_buf, sem,
):
    copies = []
    for src, outs in ((all_ref, (rq, rk, rv)), (lat_ref, (lq, lk, lv))):
        first = 0
        for out in outs:
            width = out.shape[1]
            copies.append((src.at[:, pl.ds(first, width)], out))
            first += width
    copies += [(sq_ref, cq), (sk_ref, ck), (sv_ref, cv)]
    started = []
    for i, (src, dst) in enumerate(copies):
        copy = pltpu.make_async_copy(src, dst, sem.at[i])
        copy.start()
        started.append(copy)
    norm_buf[...] = norm_ref[...].astype(jnp.bfloat16)
    copy = pltpu.make_async_copy(norm_buf, norm_out, sem.at[len(copies)])
    copy.start()
    for done in started:
        done.wait()
    copy.wait()


def body(tq, sq, tk, sk, tv, sv, nt, ns):
    f32, bf16 = jnp.float32, jnp.bfloat16
    anyspace = pl.BlockSpec(memory_space=pl.ANY)
    hbm = pl.BlockSpec(memory_space=pltpu.HBM)
    dma = pltpu.SemaphoreType.DMA
    norm_rows = NZERO * NW * NORM // 128
    gathered = pl.pallas_call(
        gather_kernel,
        name="gather",
        out_shape=(
            jax.ShapeDtypeStruct((NZERO * ROWS, COLS), bf16),
            jax.ShapeDtypeStruct((ROWS, COLS), f32),
            jax.ShapeDtypeStruct((WQ // 128, 128), f32),
            jax.ShapeDtypeStruct((1, WK), f32),
            jax.ShapeDtypeStruct((1, WK), f32),
            jax.ShapeDtypeStruct((norm_rows, 128), f32),
        ),
        in_specs=[hbm] * 8,
        out_specs=(pl.BlockSpec(memory_space=pltpu.VMEM),) * 6,
        scratch_shapes=[
            pltpu.VMEM((ROWS, COLS), f32),
            pltpu.VMEM((ROWS, COLS), f32),
            pltpu.VMEM((NZERO, 1, COLS), f32),
            pltpu.VMEM((NORM,), f32),
            pltpu.VMEM((NORM,), f32),
            pltpu.VMEM((NZERO, NW, 1, 128), f32),
            dma((4, 6)),
            dma((2,)),
            dma((NZERO,)), dma((NZERO,)),
            dma((NW,)), dma((NW,)),
            dma((NZERO,)), dma((NZERO,)),
            dma((4, len(ORDER))), dma((4, len(ORDER))),
        ],
        compiler_params=pltpu.CompilerParams(
            collective_id=0, has_side_effects=True, vmem_limit_bytes=26 * 2**20
        ),
    )(*(pltpu.with_memory_space_constraint(v, pltpu.HBM) for v in (tq, sq, tk, sk, tv, sv, nt, ns)))
    whole = NZERO * ROWS
    outs = pl.pallas_call(
        write_kernel,
        name="write",
        out_shape=(
            jax.ShapeDtypeStruct((whole, WQ), bf16),
            jax.ShapeDtypeStruct((whole, WK), bf16),
            jax.ShapeDtypeStruct((whole, WK), bf16),
            jax.ShapeDtypeStruct((WQ // 128, 128), f32),
            jax.ShapeDtypeStruct((1, WK), f32),
            jax.ShapeDtypeStruct((1, WK), f32),
            jax.ShapeDtypeStruct((norm_rows, 128), bf16),
            jax.ShapeDtypeStruct((ROWS, WQ), f32),
            jax.ShapeDtypeStruct((ROWS, WK), f32),
            jax.ShapeDtypeStruct((ROWS, WK), f32),
        ),
        in_specs=[anyspace] * 5 + [pl.BlockSpec(memory_space=pltpu.VMEM)],
        out_specs=(hbm,) * 10,
        scratch_shapes=[pltpu.VMEM((norm_rows, 128), bf16), dma((10,))],
        compiler_params=pltpu.CompilerParams(vmem_limit_bytes=2 * 2**20),
    )(*gathered)
    rq, rk, rv, cq, ck, cv, norm, lq, lk, lv = outs
    return (
        rq, rk, rv, cq.reshape(-1), ck.reshape(-1), cv.reshape(-1), norm.reshape(-1), lq, lk, lv
    )


def solution(mesh):
    both = P("zero", "width")
    in_specs = (both,) * 6 + (P(("zero", "width")),) * 2
    out_specs = (
        (P(None, "width"),) * 3 + (P("width"),) * 3 + (P(),) + (both,) * 3
    )
    return jax.shard_map(body, mesh=mesh, in_specs=in_specs, out_specs=out_specs, check_vma=False)
```

```python
import functools

import jax
import jax.numpy as jnp
from jax import lax
from jax.experimental import pallas as pl
from jax.experimental.pallas import tpu as pltpu
from jax.sharding import PartitionSpec as P

keep_rate = 0.5
MESH = pl.DeviceIdType.MESH

NZ, NY, NW = 4, 4, 8
NZERO = NZ * NY
ROWS = 448
WQ, WK = 896, 128
COLS = WQ + 2 * WK
QUARTER = ROWS // 4
SLAB = 16
EARLY = 16
NORM = 56

ORDER = (
    ("one", 0),
    ("two", 0, 0),
    ("one", 1),
    ("two", 1, 0),
    ("one", 2),
    ("two", 2, 0),
    ("two", 0, 1),
    ("two", 3, 0),
    ("two", 1, 1),
    ("two", 2, 1),
    ("two", 0, 2),
    ("two", 3, 1),
    ("two", 1, 2),
    ("two", 2, 2),
    ("two", 3, 2),
)
SLOT = {entry: at for at, entry in enumerate(ORDER)}
LINKS = (("y", 1), ("y", -1), ("z", 1), ("z", -1))
PARTNER = (2, 3, 0, 1)


def gather_kernel(
    tq, sq, tk, sk, tv, sv, nt, ns,
    all_ref, lat_ref, cq_ref, ck_ref, cv_ref, norm_ref,
    tbuf, sbuf, sums, ntb, nsb, nbuf, early,
    load_sem, nload_sem, sum_send, sum_recv, na_send, na_recv, nb_send, nb_recv,
    send_sem, recv_sem, early_send, early_recv,
):
    me = lax.axis_index("zero")
    wide = lax.axis_index("width")
    z, y = me // NY, me % NY

    barrier = pltpu.get_barrier_semaphore()
    for d in range(1, NZERO):
        pl.semaphore_signal(
            barrier, inc=1, device_id=(lax.rem(me + d, NZERO), wide), device_id_type=MESH
        )
    for d in range(1, NW):
        pl.semaphore_signal(
            barrier, inc=1, device_id=(me, lax.rem(wide + d, NW)), device_id_type=MESH
        )

    loads = []
    for c in range(4):
        rows = pl.ds(c * QUARTER, QUARTER)
        group = []
        for i, (src, buf, first, width) in enumerate((
            (tq, tbuf, 0, WQ), (sq, sbuf, 0, WQ),
            (tk, tbuf, WQ, WK), (sk, sbuf, WQ, WK),
            (tv, tbuf, WQ + WK, WK), (sv, sbuf, WQ + WK, WK),
        )):
            copy = pltpu.make_async_copy(
                src.at[rows], buf.at[rows, pl.ds(first, width)], load_sem.at[c, i]
            )
            copy.start()
            group.append(copy)
        loads.append(group)
    nload = (
        pltpu.make_async_copy(nt, ntb, nload_sem.at[0]),
        pltpu.make_async_copy(ns, nsb, nload_sem.at[1]),
    )
    for copy in nload:
        copy.start()

    acc = jnp.zeros((8, COLS), jnp.float32)
    for c in range(4):
        for copy in loads[c]:
            copy.wait()

        def average(i, acc):
            rows = pl.ds(pl.multiple_of(c * QUARTER + i * SLAB, SLAB), SLAB)
            latest = keep_rate * sbuf[rows, :] + (1.0 - keep_rate) * tbuf[rows, :]
            lat_ref[rows, :] = latest
            square = latest * latest
            return acc + square[:8] + square[8:]

        acc = lax.fori_loop(0, QUARTER // SLAB, average, acc)
    sums[me] = jnp.sum(acc, axis=0, keepdims=True)
    for copy in nload:
        copy.wait()
    mine = (ntb[...] + nsb[...]).reshape(1, NORM)
    nbuf[me, wide] = jnp.concatenate([mine, jnp.zeros((1, 128 - NORM), jnp.float32)], axis=1)

    pl.semaphore_wait(barrier, NZERO - 1 + NW - 1)

    small = []
    for d in range(1, NZERO):
        copy = pltpu.make_async_remote_copy(
            src_ref=sums.at[me], dst_ref=sums.at[me],
            send_sem=sum_send.at[d], recv_sem=sum_recv.at[d],
            device_id=(lax.rem(me + d, NZERO), wide), device_id_type=MESH,
        )
        copy.start()
        small.append(copy)
    across = []
    for d in range(1, NW):
        copy = pltpu.make_async_remote_copy(
            src_ref=nbuf.at[me, wide], dst_ref=nbuf.at[me, wide],
            send_sem=na_send.at[d], recv_sem=na_recv.at[d],
            device_id=(me, lax.rem(wide + d, NW)), device_id_type=MESH,
        )
        copy.start()
        across.append(copy)

    def at(zz, yy):
        return lax.rem(zz + 2 * NZ, NZ) * NY + lax.rem(yy + 2 * NY, NY)

    def beside(link, steps):
        ring, sign = LINKS[link]
        return at(z + sign * steps, y) if ring == "z" else at(z, y + sign * steps)

    ahead = {}
    for which in range(2):
        for link in range(4):
            p = PARTNER[link] if which else link
            copy = pltpu.make_async_remote_copy(
                src_ref=lat_ref.at[pl.ds(p * QUARTER, EARLY)], dst_ref=early.at[link, which],
                send_sem=early_send.at[link, which], recv_sem=early_recv.at[link, which],
                device_id=(beside(link, 1), wide), device_id_type=MESH,
            )
            copy.start()
            ahead[link, which] = copy

    for copy in small:
        copy.wait()

    total = sums[0]
    for d in range(1, NZERO):
        total = total + sums[d]
    scale = jnp.sqrt(total)
    for r in range(WQ // 128):
        cq_ref[pl.ds(r, 1), :] = scale[:, r * 128 : (r + 1) * 128]
    ck_ref[...] = scale[:, WQ : WQ + WK]
    cv_ref[...] = scale[:, WQ + WK :]
    inverse = jnp.broadcast_to(1.0 / scale, (SLAB, COLS))

    copies = {}

    def piece(p, zz, yy, skip):
        first = at(zz, yy) * ROWS + p * QUARTER + skip
        return pl.ds(pl.multiple_of(first, SLAB), QUARTER - skip)

    def start(link, slot):
        ring, sign = LINKS[link]
        entry = ORDER[slot]
        if entry[0] == "one":
            p, j, k = link, 0, entry[1]
            if k > 0:
                copies[link, SLOT["one", k - 1]].wait_recv()
            steps = {ring: k}
        else:
            p, j, k = PARTNER[link], entry[1], entry[2]
            if k > 0:
                copies[link, SLOT["two", j, k - 1]].wait_recv()
            elif j == 3:
                copies[p, SLOT["one", 2]].wait_recv()
            steps = {ring: k, LINKS[p][0]: j}
        skip = 0 if any(steps.values()) else EARLY
        rows = piece(p, z - sign * steps.get("z", 0), y - sign * steps.get("y", 0), skip)
        copy = pltpu.make_async_remote_copy(
            src_ref=all_ref.at[rows], dst_ref=all_ref.at[rows],
            send_sem=send_sem.at[link, slot], recv_sem=recv_sem.at[link, slot],
            device_id=(beside(link, 1), wide), device_id_type=MESH,
        )
        copy.start()
        copies[link, slot] = copy

    def narrow(src, first, there, steps):
        def step(i, _):
            rows = pl.ds(pl.multiple_of(first + i * SLAB, SLAB), SLAB)
            out = pl.ds(pl.multiple_of(there + i * SLAB, SLAB), SLAB)
            all_ref[out, :] = (src[rows, :] * inverse).astype(jnp.bfloat16)
            return 0

        lax.fori_loop(0, steps, step, 0)

    for p in range(4):
        first = p * QUARTER + EARLY
        narrow(lat_ref, first, me * ROWS + first, (QUARTER - EARLY) // SLAB)
        start(p, 0)
    for link in range(4):
        start(link, 1)
    for p in range(4):
        first = p * QUARTER
        narrow(lat_ref, first, me * ROWS + first, EARLY // SLAB)
    for link in range(4):
        for which in range(2):
            ahead[link, which].wait()
            p = PARTNER[link] if which else link
            narrow(early.at[link, which], 0, beside(link, -1) * ROWS + p * QUARTER, EARLY // SLAB)

    for copy in across:
        copy.wait()
    on = []
    for d in range(1, NZERO):
        copy = pltpu.make_async_remote_copy(
            src_ref=nbuf.at[me], dst_ref=nbuf.at[me],
            send_sem=nb_send.at[d], recv_sem=nb_recv.at[d],
            device_id=(lax.rem(me + d, NZERO), wide), device_id_type=MESH,
        )
        copy.start()
        on.append(copy)

    for slot in range(2, 6):
        for link in range(4):
            start(link, slot)

    for copy in on:
        copy.wait()
    lane = lax.broadcasted_iota(jnp.int32, (1, 128), 1)
    for r in range(NZERO * NW * NORM // 128):
        row = jnp.zeros((1, 128), jnp.float32)
        for d in range(128 * r // NORM, (128 * r + 127) // NORM + 1):
            shift = d * NORM - 128 * r
            moved = pltpu.roll(nbuf[d // NW, d % NW], shift % 128, 1)
            row = jnp.where((lane >= shift) & (lane < shift + NORM), moved, row)
        norm_ref[pl.ds(r, 1), :] = row

    for slot in range(6, len(ORDER)):
        for link in range(4):
            start(link, slot)

    for slot in range(len(ORDER)):
        for link in range(4):
            copies[link, slot].wait_send()
    waited = {("one", 0), ("one", 1), ("one", 2)}
    waited |= {("two", j, k) for j in range(4) for k in range(2)}
    for entry in ORDER:
        if entry not in waited:
            for link in range(4):
                copies[link, SLOT[entry]].wait_recv()


def write_kernel(
    all_ref, lat_ref, sq_ref, sk_ref, sv_ref, norm_ref,
    rq, rk, rv, cq, ck, cv, norm_out, lq, lk, lv,
    norm_buf, sem,
):
    copies = []
    for src, outs in ((all_ref, (rq, rk, rv)), (lat_ref, (lq, lk, lv))):
        first = 0
        for out in outs:
            width = out.shape[1]
            copies.append((src.at[:, pl.ds(first, width)], out))
            first += width
    copies += [(sq_ref, cq), (sk_ref, ck), (sv_ref, cv)]
    started = []
    for i, (src, dst) in enumerate(copies):
        copy = pltpu.make_async_copy(src, dst, sem.at[i])
        copy.start()
        started.append(copy)
    norm_buf[...] = norm_ref[...].astype(jnp.bfloat16)
    copy = pltpu.make_async_copy(norm_buf, norm_out, sem.at[len(copies)])
    copy.start()
    for done in started:
        done.wait()
    copy.wait()


def body(tq, sq, tk, sk, tv, sv, nt, ns):
    f32, bf16 = jnp.float32, jnp.bfloat16
    anyspace = pl.BlockSpec(memory_space=pl.ANY)
    hbm = pl.BlockSpec(memory_space=pltpu.HBM)
    dma = pltpu.SemaphoreType.DMA
    norm_rows = NZERO * NW * NORM // 128
    gathered = pl.pallas_call(
        gather_kernel,
        name="gather",
        out_shape=(
            jax.ShapeDtypeStruct((NZERO * ROWS, COLS), bf16),
            jax.ShapeDtypeStruct((ROWS, COLS), f32),
            jax.ShapeDtypeStruct((WQ // 128, 128), f32),
            jax.ShapeDtypeStruct((1, WK), f32),
            jax.ShapeDtypeStruct((1, WK), f32),
            jax.ShapeDtypeStruct((norm_rows, 128), f32),
        ),
        in_specs=[hbm] * 8,
        out_specs=(pl.BlockSpec(memory_space=pltpu.VMEM),) * 6,
        scratch_shapes=[
            pltpu.VMEM((ROWS, COLS), f32),
            pltpu.VMEM((ROWS, COLS), f32),
            pltpu.VMEM((NZERO, 1, COLS), f32),
            pltpu.VMEM((NORM,), f32),
            pltpu.VMEM((NORM,), f32),
            pltpu.VMEM((NZERO, NW, 1, 128), f32),
            pltpu.VMEM((4, 2, EARLY, COLS), f32),
            dma((4, 6)),
            dma((2,)),
            dma((NZERO,)), dma((NZERO,)),
            dma((NW,)), dma((NW,)),
            dma((NZERO,)), dma((NZERO,)),
            dma((4, len(ORDER))), dma((4, len(ORDER))),
            dma((4, 2)), dma((4, 2)),
        ],
        compiler_params=pltpu.CompilerParams(
            collective_id=0, has_side_effects=True, vmem_limit_bytes=26 * 2**20
        ),
    )(*(pltpu.with_memory_space_constraint(v, pltpu.HBM) for v in (tq, sq, tk, sk, tv, sv, nt, ns)))
    whole = NZERO * ROWS
    outs = pl.pallas_call(
        write_kernel,
        name="write",
        out_shape=(
            jax.ShapeDtypeStruct((whole, WQ), bf16),
            jax.ShapeDtypeStruct((whole, WK), bf16),
            jax.ShapeDtypeStruct((whole, WK), bf16),
            jax.ShapeDtypeStruct((WQ // 128, 128), f32),
            jax.ShapeDtypeStruct((1, WK), f32),
            jax.ShapeDtypeStruct((1, WK), f32),
            jax.ShapeDtypeStruct((norm_rows, 128), bf16),
            jax.ShapeDtypeStruct((ROWS, WQ), f32),
            jax.ShapeDtypeStruct((ROWS, WK), f32),
            jax.ShapeDtypeStruct((ROWS, WK), f32),
        ),
        in_specs=[anyspace] * 5 + [pl.BlockSpec(memory_space=pltpu.VMEM)],
        out_specs=(hbm,) * 10,
        scratch_shapes=[pltpu.VMEM((norm_rows, 128), bf16), dma((10,))],
        compiler_params=pltpu.CompilerParams(vmem_limit_bytes=2 * 2**20),
    )(*gathered)
    rq, rk, rv, cq, ck, cv, norm, lq, lk, lv = outs
    return (
        rq, rk, rv, cq.reshape(-1), ck.reshape(-1), cv.reshape(-1), norm.reshape(-1), lq, lk, lv
    )


def solution(mesh):
    both = P("zero", "width")
    in_specs = (both,) * 6 + (P(("zero", "width")),) * 2
    out_specs = (
        (P(None, "width"),) * 3 + (P("width"),) * 3 + (P(),) + (both,) * 3
    )
    return jax.shard_map(body, mesh=mesh, in_specs=in_specs, out_specs=out_specs, check_vma=False)
```

```python
import functools

import jax
import jax.numpy as jnp
from jax import lax
from jax.experimental import pallas as pl
from jax.experimental.pallas import tpu as pltpu
from jax.sharding import PartitionSpec as P

keep_rate = 0.5
MESH = pl.DeviceIdType.MESH

NZ, NY, NW = 4, 4, 8
NZERO = NZ * NY
ROWS = 448
WQ, WK = 896, 128
COLS = WQ + 2 * WK
QUARTER = ROWS // 4
SLAB = 16
EARLY = 16
NORM = 56

ORDER = (
    ("one", 0),
    ("two", 0, 0),
    ("one", 1),
    ("two", 1, 0),
    ("one", 2),
    ("two", 2, 0),
    ("two", 0, 1),
    ("two", 3, 0),
    ("two", 1, 1),
    ("two", 2, 1),
    ("two", 0, 2),
    ("two", 3, 1),
    ("two", 1, 2),
    ("two", 2, 2),
    ("two", 3, 2),
)
SLOT = {entry: at for at, entry in enumerate(ORDER)}
LINKS = (("y", 1), ("y", -1), ("z", 1), ("z", -1))
PARTNER = (2, 3, 0, 1)


def gather_kernel(
    tq, sq, tk, sk, tv, sv, nt, ns,
    all_ref, lat_ref, cq_ref, ck_ref, cv_ref, norm_ref,
    tbuf, sbuf, sums, ntb, nsb, nbuf, early,
    load_sem, nload_sem, sum_send, sum_recv, na_send, na_recv, nb_send, nb_recv,
    send_sem, recv_sem, early_send, early_recv, group_sem, go_sem,
):
    me = lax.axis_index("zero")
    wide = lax.axis_index("width")
    z, y = me // NY, me % NY

    barrier = pltpu.get_barrier_semaphore()
    for d in range(1, NZERO):
        pl.semaphore_signal(
            barrier, inc=1, device_id=(lax.rem(me + d, NZERO), wide), device_id_type=MESH
        )

    @pl.when(me == 0)
    def _():
        for d in range(1, NW):
            pl.semaphore_signal(
                barrier, inc=1, device_id=(me, lax.rem(wide + d, NW)), device_id_type=MESH
            )

    loads = []
    for c in range(4):
        rows = pl.ds(c * QUARTER, QUARTER)
        group = []
        for i, (src, buf, first, width) in enumerate((
            (tq, tbuf, 0, WQ), (sq, sbuf, 0, WQ),
            (tk, tbuf, WQ, WK), (sk, sbuf, WQ, WK),
            (tv, tbuf, WQ + WK, WK), (sv, sbuf, WQ + WK, WK),
        )):
            copy = pltpu.make_async_copy(
                src.at[rows], buf.at[rows, pl.ds(first, width)], load_sem.at[c, i]
            )
            copy.start()
            group.append(copy)
        loads.append(group)
    nload = (
        pltpu.make_async_copy(nt, ntb, nload_sem.at[0]),
        pltpu.make_async_copy(ns, nsb, nload_sem.at[1]),
    )
    for copy in nload:
        copy.start()

    acc = jnp.zeros((8, COLS), jnp.float32)
    for c in range(4):
        for copy in loads[c]:
            copy.wait()

        def average(i, acc):
            rows = pl.ds(pl.multiple_of(c * QUARTER + i * SLAB, SLAB), SLAB)
            latest = keep_rate * sbuf[rows, :] + (1.0 - keep_rate) * tbuf[rows, :]
            lat_ref[rows, :] = latest
            square = latest * latest
            return acc + square[:8] + square[8:]

        acc = lax.fori_loop(0, QUARTER // SLAB, average, acc)
    sums[me] = jnp.sum(acc, axis=0, keepdims=True)

    @pl.when(me == 0)
    def _():
        pl.semaphore_wait(barrier, NZERO - 1 + NW - 1)

    @pl.when(me != 0)
    def _():
        pl.semaphore_wait(barrier, NZERO - 1)

    small = []
    for d in range(1, NZERO):
        copy = pltpu.make_async_remote_copy(
            src_ref=sums.at[me], dst_ref=sums.at[me],
            send_sem=sum_send.at[d], recv_sem=sum_recv.at[d],
            device_id=(lax.rem(me + d, NZERO), wide), device_id_type=MESH,
        )
        copy.start()
        small.append(copy)
    def at(zz, yy):
        return lax.rem(zz + 2 * NZ, NZ) * NY + lax.rem(yy + 2 * NY, NY)

    def beside(link, steps):
        ring, sign = LINKS[link]
        return at(z + sign * steps, y) if ring == "z" else at(z, y + sign * steps)

    ahead = {}
    for which in range(2):
        for link in range(4):
            p = PARTNER[link] if which else link
            copy = pltpu.make_async_remote_copy(
                src_ref=lat_ref.at[pl.ds(p * QUARTER, EARLY)], dst_ref=early.at[link, which],
                send_sem=early_send.at[link, which], recv_sem=early_recv.at[link, which],
                device_id=(beside(link, 1), wide), device_id_type=MESH,
            )
            copy.start()
            ahead[link, which] = copy

    @pl.when(me == 0)
    def _():
        for d in range(1, NW):
            pl.semaphore_signal(
                group_sem, inc=1, device_id=(me, lax.rem(wide + d, NW)), device_id_type=MESH
            )

    for copy in nload:
        copy.wait()
    mine = (ntb[...] + nsb[...]).reshape(1, NORM)
    nbuf[me, wide] = jnp.concatenate([mine, jnp.zeros((1, 128 - NORM), jnp.float32)], axis=1)

    for copy in small:
        copy.wait()

    total = sums[0]
    for d in range(1, NZERO):
        total = total + sums[d]
    scale = jnp.sqrt(total)
    for r in range(WQ // 128):
        cq_ref[pl.ds(r, 1), :] = scale[:, r * 128 : (r + 1) * 128]
    ck_ref[...] = scale[:, WQ : WQ + WK]
    cv_ref[...] = scale[:, WQ + WK :]
    inverse = jnp.broadcast_to(1.0 / scale, (SLAB, COLS))

    copies = {}

    def piece(p, zz, yy, skip):
        first = at(zz, yy) * ROWS + p * QUARTER + skip
        return pl.ds(pl.multiple_of(first, SLAB), QUARTER - skip)

    def start(link, slot):
        ring, sign = LINKS[link]
        entry = ORDER[slot]
        if entry[0] == "one":
            p, j, k = link, 0, entry[1]
            if k > 0:
                copies[link, SLOT["one", k - 1]].wait_recv()
            steps = {ring: k}
        else:
            p, j, k = PARTNER[link], entry[1], entry[2]
            if k > 0:
                copies[link, SLOT["two", j, k - 1]].wait_recv()
            elif j == 3:
                copies[p, SLOT["one", 2]].wait_recv()
            steps = {ring: k, LINKS[p][0]: j}
        skip = 0 if any(steps.values()) else EARLY
        rows = piece(p, z - sign * steps.get("z", 0), y - sign * steps.get("y", 0), skip)
        copy = pltpu.make_async_remote_copy(
            src_ref=all_ref.at[rows], dst_ref=all_ref.at[rows],
            send_sem=send_sem.at[link, slot], recv_sem=recv_sem.at[link, slot],
            device_id=(beside(link, 1), wide), device_id_type=MESH,
        )
        copy.start()
        copies[link, slot] = copy

    def narrow(src, first, there, steps):
        def step(i, _):
            rows = pl.ds(pl.multiple_of(first + i * SLAB, SLAB), SLAB)
            out = pl.ds(pl.multiple_of(there + i * SLAB, SLAB), SLAB)
            all_ref[out, :] = (src[rows, :] * inverse).astype(jnp.bfloat16)
            return 0

        lax.fori_loop(0, steps, step, 0)

    for p in range(4):
        first = p * QUARTER + EARLY
        narrow(lat_ref, first, me * ROWS + first, (QUARTER - EARLY) // SLAB)
        start(p, 0)
    for link in range(4):
        start(link, 1)
    for p in range(4):
        first = p * QUARTER
        narrow(lat_ref, first, me * ROWS + first, EARLY // SLAB)
    for link in range(4):
        for which in range(2):
            ahead[link, which].wait()
            p = PARTNER[link] if which else link
            narrow(early.at[link, which], 0, beside(link, -1) * ROWS + p * QUARTER, EARLY // SLAB)

    for slot in range(2, 4):
        for link in range(4):
            start(link, slot)

    @pl.when(me == 0)
    def _():
        pl.semaphore_wait(group_sem, NW - 1)
        for d in range(1, NZERO):
            pl.semaphore_signal(go_sem, inc=1, device_id=(d, wide), device_id_type=MESH)

    @pl.when(me != 0)
    def _():
        pl.semaphore_wait(go_sem, 1)

    across = []
    for d in range(1, NW):
        copy = pltpu.make_async_remote_copy(
            src_ref=nbuf.at[me, wide], dst_ref=nbuf.at[me, wide],
            send_sem=na_send.at[d], recv_sem=na_recv.at[d],
            device_id=(me, lax.rem(wide + d, NW)), device_id_type=MESH,
        )
        copy.start()
        across.append(copy)

    for slot in range(4, 6):
        for link in range(4):
            start(link, slot)

    for copy in across:
        copy.wait()
    on = []
    for d in range(1, NZERO):
        copy = pltpu.make_async_remote_copy(
            src_ref=nbuf.at[me], dst_ref=nbuf.at[me],
            send_sem=nb_send.at[d], recv_sem=nb_recv.at[d],
            device_id=(lax.rem(me + d, NZERO), wide), device_id_type=MESH,
        )
        copy.start()
        on.append(copy)

    for slot in range(6, 8):
        for link in range(4):
            start(link, slot)

    for copy in on:
        copy.wait()
    lane = lax.broadcasted_iota(jnp.int32, (1, 128), 1)
    for r in range(NZERO * NW * NORM // 128):
        row = jnp.zeros((1, 128), jnp.float32)
        for d in range(128 * r // NORM, (128 * r + 127) // NORM + 1):
            shift = d * NORM - 128 * r
            moved = pltpu.roll(nbuf[d // NW, d % NW], shift % 128, 1)
            row = jnp.where((lane >= shift) & (lane < shift + NORM), moved, row)
        norm_ref[pl.ds(r, 1), :] = row

    for slot in range(8, len(ORDER)):
        for link in range(4):
            start(link, slot)

    for slot in range(len(ORDER)):
        for link in range(4):
            copies[link, slot].wait_send()
    waited = {("one", 0), ("one", 1), ("one", 2)}
    waited |= {("two", j, k) for j in range(4) for k in range(2)}
    for entry in ORDER:
        if entry not in waited:
            for link in range(4):
                copies[link, SLOT[entry]].wait_recv()


def write_kernel(
    all_ref, lat_ref, sq_ref, sk_ref, sv_ref, norm_ref,
    rq, rk, rv, cq, ck, cv, norm_out, lq, lk, lv,
    norm_buf, sem,
):
    copies = []
    for src, outs in ((all_ref, (rq, rk, rv)), (lat_ref, (lq, lk, lv))):
        first = 0
        for out in outs:
            width = out.shape[1]
            copies.append((src.at[:, pl.ds(first, width)], out))
            first += width
    copies += [(sq_ref, cq), (sk_ref, ck), (sv_ref, cv)]
    started = []
    for i, (src, dst) in enumerate(copies):
        copy = pltpu.make_async_copy(src, dst, sem.at[i])
        copy.start()
        started.append(copy)
    norm_buf[...] = norm_ref[...].astype(jnp.bfloat16)
    copy = pltpu.make_async_copy(norm_buf, norm_out, sem.at[len(copies)])
    copy.start()
    for done in started:
        done.wait()
    copy.wait()


def body(tq, sq, tk, sk, tv, sv, nt, ns):
    f32, bf16 = jnp.float32, jnp.bfloat16
    anyspace = pl.BlockSpec(memory_space=pl.ANY)
    hbm = pl.BlockSpec(memory_space=pltpu.HBM)
    dma = pltpu.SemaphoreType.DMA
    norm_rows = NZERO * NW * NORM // 128
    gathered = pl.pallas_call(
        gather_kernel,
        name="gather",
        out_shape=(
            jax.ShapeDtypeStruct((NZERO * ROWS, COLS), bf16),
            jax.ShapeDtypeStruct((ROWS, COLS), f32),
            jax.ShapeDtypeStruct((WQ // 128, 128), f32),
            jax.ShapeDtypeStruct((1, WK), f32),
            jax.ShapeDtypeStruct((1, WK), f32),
            jax.ShapeDtypeStruct((norm_rows, 128), f32),
        ),
        in_specs=[hbm] * 8,
        out_specs=(pl.BlockSpec(memory_space=pltpu.VMEM),) * 6,
        scratch_shapes=[
            pltpu.VMEM((ROWS, COLS), f32),
            pltpu.VMEM((ROWS, COLS), f32),
            pltpu.VMEM((NZERO, 1, COLS), f32),
            pltpu.VMEM((NORM,), f32),
            pltpu.VMEM((NORM,), f32),
            pltpu.VMEM((NZERO, NW, 1, 128), f32),
            pltpu.VMEM((4, 2, EARLY, COLS), f32),
            dma((4, 6)),
            dma((2,)),
            dma((NZERO,)), dma((NZERO,)),
            dma((NW,)), dma((NW,)),
            dma((NZERO,)), dma((NZERO,)),
            dma((4, len(ORDER))), dma((4, len(ORDER))),
            dma((4, 2)), dma((4, 2)),
            pltpu.SemaphoreType.REGULAR, pltpu.SemaphoreType.REGULAR,
        ],
        compiler_params=pltpu.CompilerParams(
            collective_id=0, has_side_effects=True, vmem_limit_bytes=26 * 2**20
        ),
    )(*(pltpu.with_memory_space_constraint(v, pltpu.HBM) for v in (tq, sq, tk, sk, tv, sv, nt, ns)))
    whole = NZERO * ROWS
    outs = pl.pallas_call(
        write_kernel,
        name="write",
        out_shape=(
            jax.ShapeDtypeStruct((whole, WQ), bf16),
            jax.ShapeDtypeStruct((whole, WK), bf16),
            jax.ShapeDtypeStruct((whole, WK), bf16),
            jax.ShapeDtypeStruct((WQ // 128, 128), f32),
            jax.ShapeDtypeStruct((1, WK), f32),
            jax.ShapeDtypeStruct((1, WK), f32),
            jax.ShapeDtypeStruct((norm_rows, 128), bf16),
            jax.ShapeDtypeStruct((ROWS, WQ), f32),
            jax.ShapeDtypeStruct((ROWS, WK), f32),
            jax.ShapeDtypeStruct((ROWS, WK), f32),
        ),
        in_specs=[anyspace] * 5 + [pl.BlockSpec(memory_space=pltpu.VMEM)],
        out_specs=(hbm,) * 10,
        scratch_shapes=[pltpu.VMEM((norm_rows, 128), bf16), dma((10,))],
        compiler_params=pltpu.CompilerParams(vmem_limit_bytes=2 * 2**20),
    )(*gathered)
    rq, rk, rv, cq, ck, cv, norm, lq, lk, lv = outs
    return (
        rq, rk, rv, cq.reshape(-1), ck.reshape(-1), cv.reshape(-1), norm.reshape(-1), lq, lk, lv
    )


def solution(mesh):
    both = P("zero", "width")
    in_specs = (both,) * 6 + (P(("zero", "width")),) * 2
    out_specs = (
        (P(None, "width"),) * 3 + (P("width"),) * 3 + (P(),) + (both,) * 3
    )
    return jax.shard_map(body, mesh=mesh, in_specs=in_specs, out_specs=out_specs, check_vma=False)
```

```python
import functools

import jax
import jax.numpy as jnp
from jax import lax
from jax.experimental import pallas as pl
from jax.experimental.pallas import tpu as pltpu
from jax.sharding import PartitionSpec as P

keep_rate = 0.5
MESH = pl.DeviceIdType.MESH

NZ, NY, NW = 4, 4, 8
NZERO = NZ * NY
ROWS = 448
WQ, WK = 896, 128
COLS = WQ + 2 * WK
QUARTER = ROWS // 4
SLAB = 16
EARLY = 16
NORM = 56

ORDER = (
    ("one", 0),
    ("two", 0, 0),
    ("one", 1),
    ("two", 1, 0),
    ("one", 2),
    ("two", 2, 0),
    ("two", 0, 1),
    ("two", 3, 0),
    ("two", 1, 1),
    ("two", 2, 1),
    ("two", 0, 2),
    ("two", 3, 1),
    ("two", 1, 2),
    ("two", 2, 2),
    ("two", 3, 2),
)
GROUPS = (
    (2, (("one", 0),)),
    (4, (("one", 1),)),
    (6, (("two", 0, 0), ("one", 2))),
    (8, (("two", 1, 0), ("two", 2, 0))),
    (10, (("two", 0, 1), ("two", 3, 0))),
    (12, (("two", 1, 1), ("two", 2, 1))),
    (14, (("two", 3, 1),)),
)
GROUP = {entry: g for g, (_, entries) in enumerate(GROUPS) for entry in entries}
FIRST = (("one", 0), ("two", 0, 0))
OTHERS = sorted(
    ((dz, dy) for dz in range(NZ) for dy in range(NY) if dz or dy),
    key=lambda d: -min(d[0], NZ - d[0]) - min(d[1], NY - d[1]),
)
LINKS = (("y", 1), ("y", -1), ("z", 1), ("z", -1))
PARTNER = (2, 3, 0, 1)


def gather_kernel(
    tq, sq, tk, sk, tv, sv, nt, ns,
    all_ref, lat_ref, cq_ref, ck_ref, cv_ref, norm_ref,
    inbuf, sums, ntb, nsb, nbuf, early,
    load_sem, nload_sem, sum_send, sum_recv, na_send, na_recv, nb_send, nb_recv,
    send_sem, recv_sem, last_sem, early_send, early_recv, group_sem, go_sem,
):
    me = lax.axis_index("zero")
    wide = lax.axis_index("width")
    z, y = me // NY, me % NY

    def at(zz, yy):
        return lax.rem(zz + 2 * NZ, NZ) * NY + lax.rem(yy + 2 * NY, NY)

    def drain(ref, sem):
        pltpu.make_async_copy(ref, ref, sem).wait()

    barrier = pltpu.get_barrier_semaphore()
    for dz, dy in OTHERS:
        pl.semaphore_signal(
            barrier, inc=1, device_id=(at(z + dz, y + dy), wide), device_id_type=MESH
        )

    @pl.when(me == 0)
    def _():
        for d in range(1, NW):
            pl.semaphore_signal(
                barrier, inc=1, device_id=(me, lax.rem(wide + d, NW)), device_id_type=MESH
            )

    for c in range(4):
        rows = pl.ds(c * QUARTER, QUARTER)
        for i, (src, first, width) in enumerate((
            (tq, 0, WQ), (sq, 0, WQ), (tk, WQ, WK), (sk, WQ, WK), (tv, WQ + WK, WK), (sv, WQ + WK, WK)
        )):
            pltpu.make_async_copy(
                src.at[rows], inbuf.at[i % 2, rows, pl.ds(first, width)], load_sem.at[c]
            ).start()
    nload = (
        pltpu.make_async_copy(nt, ntb, nload_sem.at[0]),
        pltpu.make_async_copy(ns, nsb, nload_sem.at[1]),
    )
    for copy in nload:
        copy.start()

    acc = jnp.zeros((8, COLS), jnp.float32)
    for c in range(4):
        drain(inbuf.at[:, pl.ds(c * QUARTER, QUARTER)], load_sem.at[c])

        def average(i, acc):
            rows = pl.ds(pl.multiple_of(c * QUARTER + i * SLAB, SLAB), SLAB)
            latest = keep_rate * inbuf[1, rows, :] + (1.0 - keep_rate) * inbuf[0, rows, :]
            lat_ref[rows, :] = latest
            square = latest * latest
            return acc + square[:8] + square[8:]

        acc = lax.fori_loop(0, QUARTER // SLAB, average, acc)
    sums[me] = jnp.sum(acc, axis=0, keepdims=True)

    @pl.when(me == 0)
    def _():
        pl.semaphore_wait(barrier, NZERO - 1 + NW - 1)

    @pl.when(me != 0)
    def _():
        pl.semaphore_wait(barrier, NZERO - 1)

    for dz, dy in OTHERS:
        pltpu.make_async_remote_copy(
            src_ref=sums.at[me], dst_ref=sums.at[me], send_sem=sum_send, recv_sem=sum_recv,
            device_id=(at(z + dz, y + dy), wide), device_id_type=MESH,
        ).start()

    def beside(link, steps):
        ring, sign = LINKS[link]
        return at(z + sign * steps, y) if ring == "z" else at(z, y + sign * steps)

    for which in range(2):
        for link in range(4):
            p = PARTNER[link] if which else link
            pltpu.make_async_remote_copy(
                src_ref=lat_ref.at[pl.ds(p * QUARTER, EARLY)], dst_ref=early.at[link, which],
                send_sem=early_send, recv_sem=early_recv,
                device_id=(beside(link, 1), wide), device_id_type=MESH,
            ).start()

    @pl.when(me == 0)
    def _():
        for d in range(1, NW):
            pl.semaphore_signal(
                group_sem, inc=1, device_id=(me, lax.rem(wide + d, NW)), device_id_type=MESH
            )

    for copy in nload:
        copy.wait()
    mine = (ntb[...] + nsb[...]).reshape(1, NORM)
    nbuf[me, wide] = jnp.concatenate([mine, jnp.zeros((1, 128 - NORM), jnp.float32)], axis=1)

    some = sums.at[pl.ds(0, NZERO - 1)]
    drain(some, sum_send)
    drain(some, sum_recv)

    total = sums[0]
    for d in range(1, NZERO):
        total = total + sums[d]
    scale = jnp.sqrt(total)
    for r in range(WQ // 128):
        cq_ref[pl.ds(r, 1), :] = scale[:, r * 128 : (r + 1) * 128]
    ck_ref[...] = scale[:, WQ : WQ + WK]
    cv_ref[...] = scale[:, WQ + WK :]
    inverse = jnp.broadcast_to(1.0 / scale, (SLAB, COLS))

    def piece(p, zz, yy, skip):
        first = at(zz, yy) * ROWS + p * QUARTER + skip
        return pl.ds(pl.multiple_of(first, SLAB), QUARTER - skip)

    def count(entry):
        return QUARTER - EARLY if entry in FIRST else QUARTER

    def start(link, slot):
        ring, sign = LINKS[link]
        entry = ORDER[slot]
        for g, (when, entries) in enumerate(GROUPS):
            if when == slot:
                drain(all_ref.at[pl.ds(0, sum(map(count, entries)))], recv_sem.at[link, g])
        if entry[0] == "one":
            p, steps = link, {ring: entry[1]}
        else:
            p = PARTNER[link]
            steps = {ring: entry[2], LINKS[p][0]: entry[1]}
        skip = QUARTER - count(entry)
        rows = piece(p, z - sign * steps.get("z", 0), y - sign * steps.get("y", 0), skip)
        arrived = recv_sem.at[link, GROUP[entry]] if entry in GROUP else last_sem
        pltpu.make_async_remote_copy(
            src_ref=all_ref.at[rows], dst_ref=all_ref.at[rows], send_sem=send_sem, recv_sem=arrived,
            device_id=(beside(link, 1), wide), device_id_type=MESH,
        ).start()

    def narrow(src, first, there, steps):
        def step(i, _):
            rows = pl.ds(pl.multiple_of(first + i * SLAB, SLAB), SLAB)
            out = pl.ds(pl.multiple_of(there + i * SLAB, SLAB), SLAB)
            all_ref[out, :] = (src[rows, :] * inverse).astype(jnp.bfloat16)
            return 0

        lax.fori_loop(0, steps, step, 0)

    for p in range(4):
        first = p * QUARTER + EARLY
        narrow(lat_ref, first, me * ROWS + first, (QUARTER - EARLY) // SLAB)
        start(p, 0)
    for link in range(4):
        start(link, 1)
    for p in range(4):
        first = p * QUARTER
        narrow(lat_ref, first, me * ROWS + first, EARLY // SLAB)
    drain(early, early_send)
    drain(early, early_recv)
    for link in range(4):
        for which in range(2):
            p = PARTNER[link] if which else link
            narrow(early.at[link, which], 0, beside(link, -1) * ROWS + p * QUARTER, EARLY // SLAB)

    for slot in range(2, 4):
        for link in range(4):
            start(link, slot)

    @pl.when(me == 0)
    def _():
        pl.semaphore_wait(group_sem, NW - 1)
        for d in range(1, NZERO):
            pl.semaphore_signal(go_sem, inc=1, device_id=(d, wide), device_id_type=MESH)

    @pl.when(me != 0)
    def _():
        pl.semaphore_wait(go_sem, 1)

    for d in range(1, NW):
        pltpu.make_async_remote_copy(
            src_ref=nbuf.at[me, wide], dst_ref=nbuf.at[me, wide], send_sem=na_send, recv_sem=na_recv,
            device_id=(me, lax.rem(wide + d, NW)), device_id_type=MESH,
        ).start()

    for slot in range(4, 6):
        for link in range(4):
            start(link, slot)

    row = nbuf.at[me, pl.ds(0, NW - 1)]
    drain(row, na_send)
    drain(row, na_recv)
    for dz, dy in OTHERS:
        pltpu.make_async_remote_copy(
            src_ref=nbuf.at[me], dst_ref=nbuf.at[me], send_sem=nb_send, recv_sem=nb_recv,
            device_id=(at(z + dz, y + dy), wide), device_id_type=MESH,
        ).start()

    for slot in range(6, 8):
        for link in range(4):
            start(link, slot)

    some = nbuf.at[pl.ds(0, NZERO - 1)]
    drain(some, nb_send)
    drain(some, nb_recv)
    lane = lax.broadcasted_iota(jnp.int32, (1, 128), 1)
    for r in range(NZERO * NW * NORM // 128):
        row = jnp.zeros((1, 128), jnp.float32)
        for d in range(128 * r // NORM, (128 * r + 127) // NORM + 1):
            shift = d * NORM - 128 * r
            moved = pltpu.roll(nbuf[d // NW, d % NW], shift % 128, 1)
            row = jnp.where((lane >= shift) & (lane < shift + NORM), moved, row)
        norm_ref[pl.ds(r, 1), :] = row

    for slot in range(8, len(ORDER)):
        for link in range(4):
            start(link, slot)

    drain(all_ref.at[pl.ds(0, 4 * sum(map(count, ORDER)))], send_sem)
    drain(all_ref.at[pl.ds(0, 4 * QUARTER * (len(ORDER) - len(GROUP)))], last_sem)


def write_kernel(
    all_ref, lat_ref, sq_ref, sk_ref, sv_ref, norm_ref,
    rq, rk, rv, cq, ck, cv, norm_out, lq, lk, lv,
    norm_buf, sem,
):
    copies = []
    for src, outs in ((all_ref, (rq, rk, rv)), (lat_ref, (lq, lk, lv))):
        first = 0
        for out in outs:
            width = out.shape[1]
            copies.append((src.at[:, pl.ds(first, width)], out))
            first += width
    copies += [(sq_ref, cq), (sk_ref, ck), (sv_ref, cv)]
    started = []
    for i, (src, dst) in enumerate(copies):
        copy = pltpu.make_async_copy(src, dst, sem.at[i])
        copy.start()
        started.append(copy)
    norm_buf[...] = norm_ref[...].astype(jnp.bfloat16)
    copy = pltpu.make_async_copy(norm_buf, norm_out, sem.at[len(copies)])
    copy.start()
    for done in started:
        done.wait()
    copy.wait()


def body(tq, sq, tk, sk, tv, sv, nt, ns):
    f32, bf16 = jnp.float32, jnp.bfloat16
    anyspace = pl.BlockSpec(memory_space=pl.ANY)
    hbm = pl.BlockSpec(memory_space=pltpu.HBM)
    dma = pltpu.SemaphoreType.DMA
    norm_rows = NZERO * NW * NORM // 128
    gathered = pl.pallas_call(
        gather_kernel,
        name="gather",
        out_shape=(
            jax.ShapeDtypeStruct((NZERO * ROWS, COLS), bf16),
            jax.ShapeDtypeStruct((ROWS, COLS), f32),
            jax.ShapeDtypeStruct((WQ // 128, 128), f32),
            jax.ShapeDtypeStruct((1, WK), f32),
            jax.ShapeDtypeStruct((1, WK), f32),
            jax.ShapeDtypeStruct((norm_rows, 128), f32),
        ),
        in_specs=[hbm] * 8,
        out_specs=(pl.BlockSpec(memory_space=pltpu.VMEM),) * 6,
        scratch_shapes=[
            pltpu.VMEM((2, ROWS, COLS), f32),
            pltpu.VMEM((NZERO, 1, COLS), f32),
            pltpu.VMEM((NORM,), f32),
            pltpu.VMEM((NORM,), f32),
            pltpu.VMEM((NZERO, NW, 1, 128), f32),
            pltpu.VMEM((4, 2, EARLY, COLS), f32),
            dma((4,)),
            dma((2,)),
            dma, dma,
            dma, dma,
            dma, dma,
            dma, dma((4, len(GROUPS))), dma,
            dma, dma,
            pltpu.SemaphoreType.REGULAR, pltpu.SemaphoreType.REGULAR,
        ],
        compiler_params=pltpu.CompilerParams(
            collective_id=0, has_side_effects=True, vmem_limit_bytes=26 * 2**20
        ),
    )(*(pltpu.with_memory_space_constraint(v, pltpu.HBM) for v in (tq, sq, tk, sk, tv, sv, nt, ns)))
    whole = NZERO * ROWS
    outs = pl.pallas_call(
        write_kernel,
        name="write",
        out_shape=(
            jax.ShapeDtypeStruct((whole, WQ), bf16),
            jax.ShapeDtypeStruct((whole, WK), bf16),
            jax.ShapeDtypeStruct((whole, WK), bf16),
            jax.ShapeDtypeStruct((WQ // 128, 128), f32),
            jax.ShapeDtypeStruct((1, WK), f32),
            jax.ShapeDtypeStruct((1, WK), f32),
            jax.ShapeDtypeStruct((norm_rows, 128), bf16),
            jax.ShapeDtypeStruct((ROWS, WQ), f32),
            jax.ShapeDtypeStruct((ROWS, WK), f32),
            jax.ShapeDtypeStruct((ROWS, WK), f32),
        ),
        in_specs=[anyspace] * 5 + [pl.BlockSpec(memory_space=pltpu.VMEM)],
        out_specs=(hbm,) * 10,
        scratch_shapes=[pltpu.VMEM((norm_rows, 128), bf16), dma((10,))],
        compiler_params=pltpu.CompilerParams(vmem_limit_bytes=2 * 2**20),
    )(*gathered)
    rq, rk, rv, cq, ck, cv, norm, lq, lk, lv = outs
    return (
        rq, rk, rv, cq.reshape(-1), ck.reshape(-1), cv.reshape(-1), norm.reshape(-1), lq, lk, lv
    )


def solution(mesh):
    both = P("zero", "width")
    in_specs = (both,) * 6 + (P(("zero", "width")),) * 2
    out_specs = (
        (P(None, "width"),) * 3 + (P("width"),) * 3 + (P(),) + (both,) * 3
    )
    return jax.shard_map(body, mesh=mesh, in_specs=in_specs, out_specs=out_specs, check_vma=False)
```

```python
import functools

import jax
import jax.numpy as jnp
from jax import lax
from jax.experimental import pallas as pl
from jax.experimental.pallas import tpu as pltpu
from jax.sharding import PartitionSpec as P

keep_rate = 0.5
MESH = pl.DeviceIdType.MESH

NZ, NY, NW = 4, 4, 8
NZERO = NZ * NY
ROWS = 448
WQ, WK = 896, 128
COLS = WQ + 2 * WK
QUARTER = ROWS // 4
SLAB = 16
EARLY = 16
NORM = 56

ORDER = (
    ("one", 0),
    ("two", 0, 0),
    ("one", 1),
    ("two", 1, 0),
    ("one", 2),
    ("two", 2, 0),
    ("two", 0, 1),
    ("two", 3, 0),
    ("two", 1, 1),
    ("two", 2, 1),
    ("two", 0, 2),
    ("two", 3, 1),
    ("two", 1, 2),
    ("two", 2, 2),
    ("two", 3, 2),
)
GROUPS = (
    (2, (("one", 0),)),
    (4, (("one", 1),)),
    (6, (("two", 0, 0), ("one", 2))),
    (8, (("two", 1, 0), ("two", 2, 0))),
    (10, (("two", 0, 1), ("two", 3, 0))),
    (12, (("two", 1, 1), ("two", 2, 1))),
    (14, (("two", 3, 1),)),
)
GROUP = {entry: g for g, (_, entries) in enumerate(GROUPS) for entry in entries}
FIRST = (("one", 0), ("two", 0, 0))
OTHERS = sorted(
    ((dz, dy) for dz in range(NZ) for dy in range(NY) if dz or dy),
    key=lambda d: -min(d[0], NZ - d[0]) - min(d[1], NY - d[1]),
)
LINKS = (("y", 1), ("y", -1), ("z", 1), ("z", -1))
PARTNER = (2, 3, 0, 1)


def gather_kernel(
    tq, sq, tk, sk, tv, sv, nt, ns,
    all_ref, lat_ref, cq_ref, ck_ref, cv_ref, norm_ref,
    inbuf, sums, ntb, nsb, nbuf, early,
    load_sem, nload_sem, sum_send, sum_recv, na_send, na_recv,
    send_sem, recv_sem, last_sem, early_send, early_recv, group_sem, go_sem,
):
    me = lax.axis_index("zero")
    wide = lax.axis_index("width")
    z, y = me // NY, me % NY

    def at(zz, yy):
        return lax.rem(zz + 2 * NZ, NZ) * NY + lax.rem(yy + 2 * NY, NY)

    def drain(ref, sem):
        pltpu.make_async_copy(ref, ref, sem).wait()

    barrier = pltpu.get_barrier_semaphore()
    for dz, dy in OTHERS:
        pl.semaphore_signal(
            barrier, inc=1, device_id=(at(z + dz, y + dy), wide), device_id_type=MESH
        )

    @pl.when(me == 0)
    def _():
        for d in range(1, NW):
            pl.semaphore_signal(
                barrier, inc=1, device_id=(me, lax.rem(wide + d, NW)), device_id_type=MESH
            )

    for c in range(4):
        rows = pl.ds(c * QUARTER, QUARTER)
        for i, (src, first, width) in enumerate((
            (tq, 0, WQ), (sq, 0, WQ), (tk, WQ, WK), (sk, WQ, WK), (tv, WQ + WK, WK), (sv, WQ + WK, WK)
        )):
            pltpu.make_async_copy(
                src.at[rows], inbuf.at[i % 2, rows, pl.ds(first, width)], load_sem.at[c]
            ).start()
    nload = (
        pltpu.make_async_copy(nt, ntb, nload_sem.at[0]),
        pltpu.make_async_copy(ns, nsb, nload_sem.at[1]),
    )
    for copy in nload:
        copy.start()

    acc = jnp.zeros((8, COLS), jnp.float32)
    for c in range(4):
        drain(inbuf.at[:, pl.ds(c * QUARTER, QUARTER)], load_sem.at[c])

        def average(i, acc):
            rows = pl.ds(pl.multiple_of(c * QUARTER + i * SLAB, SLAB), SLAB)
            latest = keep_rate * inbuf[1, rows, :] + (1.0 - keep_rate) * inbuf[0, rows, :]
            lat_ref[rows, :] = latest
            square = latest * latest
            return acc + square[:8] + square[8:]

        acc = lax.fori_loop(0, QUARTER // SLAB, average, acc)
    for copy in nload:
        copy.wait()
    gain = (ntb[...] + nsb[...]).reshape(1, NORM)
    sums[me] = jnp.concatenate(
        [jnp.sum(acc, axis=0, keepdims=True), gain, jnp.zeros((1, 128 - NORM), jnp.float32)], axis=1
    )

    @pl.when(me == 0)
    def _():
        pl.semaphore_wait(barrier, NZERO - 1 + NW - 1)

    @pl.when(me != 0)
    def _():
        pl.semaphore_wait(barrier, NZERO - 1)

    for dz, dy in OTHERS:
        pltpu.make_async_remote_copy(
            src_ref=sums.at[me], dst_ref=sums.at[me], send_sem=sum_send, recv_sem=sum_recv,
            device_id=(at(z + dz, y + dy), wide), device_id_type=MESH,
        ).start()

    def beside(link, steps):
        ring, sign = LINKS[link]
        return at(z + sign * steps, y) if ring == "z" else at(z, y + sign * steps)

    for which in range(2):
        for link in range(4):
            p = PARTNER[link] if which else link
            pltpu.make_async_remote_copy(
                src_ref=lat_ref.at[pl.ds(p * QUARTER, EARLY)], dst_ref=early.at[link, which],
                send_sem=early_send, recv_sem=early_recv,
                device_id=(beside(link, 1), wide), device_id_type=MESH,
            ).start()

    @pl.when(me == 0)
    def _():
        for d in range(1, NW):
            pl.semaphore_signal(
                group_sem, inc=1, device_id=(me, lax.rem(wide + d, NW)), device_id_type=MESH
            )

    some = sums.at[pl.ds(0, NZERO - 1)]
    drain(some, sum_send)
    drain(some, sum_recv)

    total = sums[0, :, :COLS]
    for d in range(1, NZERO):
        total = total + sums[d, :, :COLS]
    scale = jnp.sqrt(total)
    for r in range(WQ // 128):
        cq_ref[pl.ds(r, 1), :] = scale[:, r * 128 : (r + 1) * 128]
    ck_ref[...] = scale[:, WQ : WQ + WK]
    cv_ref[...] = scale[:, WQ + WK :]
    inverse = jnp.broadcast_to(1.0 / scale, (SLAB, COLS))

    def piece(p, zz, yy, skip):
        first = at(zz, yy) * ROWS + p * QUARTER + skip
        return pl.ds(pl.multiple_of(first, 8), QUARTER - skip)

    def count(entry):
        return QUARTER - EARLY if entry in FIRST else QUARTER

    def start(link, slot):
        ring, sign = LINKS[link]
        entry = ORDER[slot]
        if entry[0] == "one":
            p, steps = link, {ring: entry[1]}
        else:
            p = PARTNER[link]
            steps = {ring: entry[2], LINKS[p][0]: entry[1]}
        skip = QUARTER - count(entry)
        rows = piece(p, z - sign * steps.get("z", 0), y - sign * steps.get("y", 0), skip)
        arrived = recv_sem.at[GROUP[entry]] if entry in GROUP else last_sem
        pltpu.make_async_remote_copy(
            src_ref=all_ref.at[rows], dst_ref=all_ref.at[rows], send_sem=send_sem, recv_sem=arrived,
            device_id=(beside(link, 1), wide), device_id_type=MESH,
        ).start()

    def starts(first, last):
        for slot in range(first, last):
            for g, (when, entries) in enumerate(GROUPS):
                if when == slot:
                    drain(all_ref.at[pl.ds(0, 4 * sum(map(count, entries)))], recv_sem.at[g])
            for link in range(4):
                start(link, slot)

    def narrow(src, first, there, count):
        def some(at_row, height):
            rows = pl.ds(pl.multiple_of(first + at_row, 8), height)
            out = pl.ds(pl.multiple_of(there + at_row, 8), height)
            all_ref[out, :] = (src[rows, :] * inverse[:height]).astype(jnp.bfloat16)

        def step(i, _):
            some(i * SLAB, SLAB)
            return 0

        lax.fori_loop(0, count // SLAB, step, 0)
        if count % SLAB:
            some(count // SLAB * SLAB, count % SLAB)

    for p in range(4):
        first = p * QUARTER + EARLY
        narrow(lat_ref, first, me * ROWS + first, QUARTER - EARLY)
        start(p, 0)
    for link in range(4):
        start(link, 1)
    for p in range(4):
        first = p * QUARTER
        narrow(lat_ref, first, me * ROWS + first, EARLY)
    drain(early, early_send)
    drain(early, early_recv)
    for link in range(4):
        for which in range(2):
            p = PARTNER[link] if which else link
            narrow(early.at[link, which], 0, beside(link, -1) * ROWS + p * QUARTER, EARLY)

    starts(2, 4)

    @pl.when(me == 0)
    def _():
        pl.semaphore_wait(group_sem, NW - 1)
        for d in range(1, NZERO):
            pl.semaphore_signal(go_sem, inc=1, device_id=(d, wide), device_id_type=MESH)

    @pl.when(me != 0)
    def _():
        pl.semaphore_wait(go_sem, 1)

    nbuf[wide] = sums[:, :, COLS:]
    for d in range(1, NW):
        pltpu.make_async_remote_copy(
            src_ref=nbuf.at[wide], dst_ref=nbuf.at[wide], send_sem=na_send, recv_sem=na_recv,
            device_id=(me, lax.rem(wide + d, NW)), device_id_type=MESH,
        ).start()

    starts(4, 6)

    starts(6, 8)

    some = nbuf.at[pl.ds(0, NW - 1)]
    drain(some, na_send)
    drain(some, na_recv)
    lane = lax.broadcasted_iota(jnp.int32, (1, 128), 1)
    for r in range(NZERO * NW * NORM // 128):
        row = jnp.zeros((1, 128), jnp.float32)
        for d in range(128 * r // NORM, (128 * r + 127) // NORM + 1):
            shift = d * NORM - 128 * r
            moved = pltpu.roll(nbuf[d % NW, d // NW], shift % 128, 1)
            row = jnp.where((lane >= shift) & (lane < shift + NORM), moved, row)
        norm_ref[pl.ds(r, 1), :] = row

    starts(8, len(ORDER))

    drain(all_ref.at[pl.ds(0, 4 * sum(map(count, ORDER)))], send_sem)
    drain(all_ref.at[pl.ds(0, 4 * QUARTER * (len(ORDER) - len(GROUP)))], last_sem)


def write_kernel(
    all_ref, lat_ref, sq_ref, sk_ref, sv_ref, norm_ref,
    rq, rk, rv, cq, ck, cv, norm_out, lq, lk, lv,
    norm_buf, sem,
):
    copies = []
    for src, outs in ((all_ref, (rq, rk, rv)), (lat_ref, (lq, lk, lv))):
        first = 0
        for out in outs:
            width = out.shape[1]
            copies.append((src.at[:, pl.ds(first, width)], out))
            first += width
    copies += [(sq_ref, cq), (sk_ref, ck), (sv_ref, cv)]
    started = []
    for i, (src, dst) in enumerate(copies):
        copy = pltpu.make_async_copy(src, dst, sem.at[i])
        copy.start()
        started.append(copy)
    norm_buf[...] = norm_ref[...].astype(jnp.bfloat16)
    copy = pltpu.make_async_copy(norm_buf, norm_out, sem.at[len(copies)])
    copy.start()
    for done in started:
        done.wait()
    copy.wait()


def body(tq, sq, tk, sk, tv, sv, nt, ns):
    f32, bf16 = jnp.float32, jnp.bfloat16
    anyspace = pl.BlockSpec(memory_space=pl.ANY)
    hbm = pl.BlockSpec(memory_space=pltpu.HBM)
    dma = pltpu.SemaphoreType.DMA
    norm_rows = NZERO * NW * NORM // 128
    gathered = pl.pallas_call(
        gather_kernel,
        name="gather",
        out_shape=(
            jax.ShapeDtypeStruct((NZERO * ROWS, COLS), bf16),
            jax.ShapeDtypeStruct((ROWS, COLS), f32),
            jax.ShapeDtypeStruct((WQ // 128, 128), f32),
            jax.ShapeDtypeStruct((1, WK), f32),
            jax.ShapeDtypeStruct((1, WK), f32),
            jax.ShapeDtypeStruct((norm_rows, 128), f32),
        ),
        in_specs=[hbm] * 8,
        out_specs=(pl.BlockSpec(memory_space=pltpu.VMEM),) * 6,
        scratch_shapes=[
            pltpu.VMEM((2, ROWS, COLS), f32),
            pltpu.VMEM((NZERO, 1, COLS + 128), f32),
            pltpu.VMEM((NORM,), f32),
            pltpu.VMEM((NORM,), f32),
            pltpu.VMEM((NW, NZERO, 1, 128), f32),
            pltpu.VMEM((4, 2, EARLY, COLS), f32),
            dma((4,)),
            dma((2,)),
            dma, dma,
            dma, dma,
            dma, dma((len(GROUPS),)), dma,
            dma, dma,
            pltpu.SemaphoreType.REGULAR, pltpu.SemaphoreType.REGULAR,
        ],
        compiler_params=pltpu.CompilerParams(
            collective_id=0, has_side_effects=True, vmem_limit_bytes=26 * 2**20
        ),
    )(*(pltpu.with_memory_space_constraint(v, pltpu.HBM) for v in (tq, sq, tk, sk, tv, sv, nt, ns)))
    whole = NZERO * ROWS
    outs = pl.pallas_call(
        write_kernel,
        name="write",
        out_shape=(
            jax.ShapeDtypeStruct((whole, WQ), bf16),
            jax.ShapeDtypeStruct((whole, WK), bf16),
            jax.ShapeDtypeStruct((whole, WK), bf16),
            jax.ShapeDtypeStruct((WQ // 128, 128), f32),
            jax.ShapeDtypeStruct((1, WK), f32),
            jax.ShapeDtypeStruct((1, WK), f32),
            jax.ShapeDtypeStruct((norm_rows, 128), bf16),
            jax.ShapeDtypeStruct((ROWS, WQ), f32),
            jax.ShapeDtypeStruct((ROWS, WK), f32),
            jax.ShapeDtypeStruct((ROWS, WK), f32),
        ),
        in_specs=[anyspace] * 5 + [pl.BlockSpec(memory_space=pltpu.VMEM)],
        out_specs=(hbm,) * 10,
        scratch_shapes=[pltpu.VMEM((norm_rows, 128), bf16), dma((10,))],
        compiler_params=pltpu.CompilerParams(vmem_limit_bytes=2 * 2**20),
    )(*gathered)
    rq, rk, rv, cq, ck, cv, norm, lq, lk, lv = outs
    return (
        rq, rk, rv, cq.reshape(-1), ck.reshape(-1), cv.reshape(-1), norm.reshape(-1), lq, lk, lv
    )


def solution(mesh):
    both = P("zero", "width")
    in_specs = (both,) * 6 + (P(("zero", "width")),) * 2
    out_specs = (
        (P(None, "width"),) * 3 + (P("width"),) * 3 + (P(),) + (both,) * 3
    )
    return jax.shard_map(body, mesh=mesh, in_specs=in_specs, out_specs=out_specs, check_vma=False)
```

```python
import functools

import jax
import jax.numpy as jnp
from jax import lax
from jax.experimental import pallas as pl
from jax.experimental.pallas import tpu as pltpu
from jax.sharding import PartitionSpec as P

keep_rate = 0.5
MESH = pl.DeviceIdType.MESH

NZ, NY, NW = 4, 4, 8
NZERO = NZ * NY
ROWS = 448
WQ, WK = 896, 128
COLS = WQ + 2 * WK
QUARTER = ROWS // 4
SLAB = 16
EARLY = 16
NORM = 56

ORDER = (
    ("one", 0),
    ("two", 0, 0),
    ("one", 1),
    ("two", 1, 0),
    ("one", 2),
    ("two", 2, 0),
    ("two", 0, 1),
    ("two", 3, 0),
    ("two", 1, 1),
    ("two", 2, 1),
    ("two", 0, 2),
    ("two", 3, 1),
    ("two", 1, 2),
    ("two", 2, 2),
    ("two", 3, 2),
)
GROUPS = (
    (2, (("one", 0),)),
    (4, (("one", 1),)),
    (6, (("two", 0, 0), ("one", 2))),
    (8, (("two", 1, 0), ("two", 2, 0))),
    (10, (("two", 0, 1), ("two", 3, 0))),
    (12, (("two", 1, 1), ("two", 2, 1))),
    (14, (("two", 3, 1),)),
)
GROUP = {entry: g for g, (_, entries) in enumerate(GROUPS) for entry in entries}
FIRST = (("one", 0), ("two", 0, 0))
OTHERS = sorted(
    ((dz, dy) for dz in range(NZ) for dy in range(NY) if dz or dy),
    key=lambda d: -min(d[0], NZ - d[0]) - min(d[1], NY - d[1]),
)
LINKS = (("y", 1), ("y", -1), ("z", 1), ("z", -1))
PARTNER = (2, 3, 0, 1)


def gather_kernel(
    tq, sq, tk, sk, tv, sv, nt, ns,
    all_ref, lat_ref, cq_ref, ck_ref, cv_ref, norm_ref,
    inbuf, sums, ntb, nsb, nbuf, early,
    load_sem, nload_sem, sum_send, sum_recv, na_send, na_recv,
    send_sem, recv_sem, last_sem, early_send, early_recv, group_sem, go_sem,
):
    me = lax.axis_index("zero")
    wide = lax.axis_index("width")
    z, y = me // NY, me % NY

    def at(zz, yy):
        return lax.rem(zz + 2 * NZ, NZ) * NY + lax.rem(yy + 2 * NY, NY)

    def drain(ref, sem):
        pltpu.make_async_copy(ref, ref, sem).wait()

    barrier = pltpu.get_barrier_semaphore()
    for dz, dy in OTHERS:
        pl.semaphore_signal(
            barrier, inc=1, device_id=(at(z + dz, y + dy), wide), device_id_type=MESH
        )

    @pl.when(me == 0)
    def _():
        for d in range(1, NW):
            pl.semaphore_signal(
                barrier, inc=1, device_id=(me, lax.rem(wide + d, NW)), device_id_type=MESH
            )

    for c in range(2):
        rows = pl.ds(c * 2 * QUARTER, 2 * QUARTER)
        for i, (src, first, width) in enumerate((
            (tq, 0, WQ), (sq, 0, WQ), (tk, WQ, WK), (sk, WQ, WK), (tv, WQ + WK, WK), (sv, WQ + WK, WK)
        )):
            pltpu.make_async_copy(
                src.at[rows], inbuf.at[i % 2, rows, pl.ds(first, width)], load_sem.at[c]
            ).start()
    nload = (
        pltpu.make_async_copy(nt, ntb, nload_sem.at[0]),
        pltpu.make_async_copy(ns, nsb, nload_sem.at[1]),
    )
    for copy in nload:
        copy.start()

    acc = jnp.zeros((8, COLS), jnp.float32)
    for c in range(2):
        drain(inbuf.at[:, pl.ds(c * 2 * QUARTER, 2 * QUARTER)], load_sem.at[c])

        def average(i, acc):
            rows = pl.ds(pl.multiple_of(c * 2 * QUARTER + i * SLAB, SLAB), SLAB)
            latest = keep_rate * inbuf[1, rows, :] + (1.0 - keep_rate) * inbuf[0, rows, :]
            lat_ref[rows, :] = latest
            square = latest * latest
            return acc + square[:8] + square[8:]

        acc = lax.fori_loop(0, 2 * QUARTER // SLAB, average, acc, unroll=7)
    for copy in nload:
        copy.wait()
    gain = (ntb[...] + nsb[...]).reshape(1, NORM)
    sums[me] = jnp.concatenate(
        [jnp.sum(acc, axis=0, keepdims=True), gain, jnp.zeros((1, 128 - NORM), jnp.float32)], axis=1
    )

    @pl.when(me == 0)
    def _():
        pl.semaphore_wait(barrier, NZERO - 1 + NW - 1)

    @pl.when(me != 0)
    def _():
        pl.semaphore_wait(barrier, NZERO - 1)

    for dz, dy in OTHERS:
        pltpu.make_async_remote_copy(
            src_ref=sums.at[me], dst_ref=sums.at[me], send_sem=sum_send, recv_sem=sum_recv,
            device_id=(at(z + dz, y + dy), wide), device_id_type=MESH,
        ).start()

    def beside(link, steps):
        ring, sign = LINKS[link]
        return at(z + sign * steps, y) if ring == "z" else at(z, y + sign * steps)

    for which in range(2):
        for link in range(4):
            p = PARTNER[link] if which else link
            pltpu.make_async_remote_copy(
                src_ref=lat_ref.at[pl.ds(p * QUARTER, EARLY)], dst_ref=early.at[link, which],
                send_sem=early_send, recv_sem=early_recv,
                device_id=(beside(link, 1), wide), device_id_type=MESH,
            ).start()

    @pl.when(me == 0)
    def _():
        for d in range(1, NW):
            pl.semaphore_signal(
                group_sem, inc=1, device_id=(me, lax.rem(wide + d, NW)), device_id_type=MESH
            )

    some = sums.at[pl.ds(0, NZERO - 1)]
    drain(some, sum_send)
    drain(some, sum_recv)

    total = sums[0, :, :COLS]
    for d in range(1, NZERO):
        total = total + sums[d, :, :COLS]
    scale = jnp.sqrt(total)
    inverse = jnp.broadcast_to(1.0 / scale, (SLAB, COLS))

    def piece(p, zz, yy, skip):
        first = at(zz, yy) * ROWS + p * QUARTER + skip
        return pl.ds(pl.multiple_of(first, 8), QUARTER - skip)

    def count(entry):
        return QUARTER - EARLY if entry in FIRST else QUARTER

    def start(link, slot):
        ring, sign = LINKS[link]
        entry = ORDER[slot]
        if entry[0] == "one":
            p, steps = link, {ring: entry[1]}
        else:
            p = PARTNER[link]
            steps = {ring: entry[2], LINKS[p][0]: entry[1]}
        skip = QUARTER - count(entry)
        rows = piece(p, z - sign * steps.get("z", 0), y - sign * steps.get("y", 0), skip)
        arrived = recv_sem.at[GROUP[entry]] if entry in GROUP else last_sem
        pltpu.make_async_remote_copy(
            src_ref=all_ref.at[rows], dst_ref=all_ref.at[rows], send_sem=send_sem, recv_sem=arrived,
            device_id=(beside(link, 1), wide), device_id_type=MESH,
        ).start()

    def starts(first, last):
        for slot in range(first, last):
            for g, (when, entries) in enumerate(GROUPS):
                if when == slot:
                    drain(all_ref.at[pl.ds(0, 4 * sum(map(count, entries)))], recv_sem.at[g])
            for link in range(4):
                start(link, slot)

    def narrow(src, first, there, count):
        def some(at_row, height):
            rows = pl.ds(pl.multiple_of(first + at_row, 8), height)
            out = pl.ds(pl.multiple_of(there + at_row, 8), height)
            all_ref[out, :] = (src[rows, :] * inverse[:height]).astype(jnp.bfloat16)

        def step(i, _):
            some(i * SLAB, SLAB)
            return 0

        lax.fori_loop(0, count // SLAB, step, 0, unroll=True)
        if count % SLAB:
            some(count // SLAB * SLAB, count % SLAB)

    for p in range(4):
        first = p * QUARTER + EARLY
        narrow(lat_ref, first, me * ROWS + first, QUARTER - EARLY)
        start(p, 0)
    for link in range(4):
        start(link, 1)
    for r in range(WQ // 128):
        cq_ref[pl.ds(r, 1), :] = scale[:, r * 128 : (r + 1) * 128]
    ck_ref[...] = scale[:, WQ : WQ + WK]
    cv_ref[...] = scale[:, WQ + WK :]
    for p in range(4):
        first = p * QUARTER
        narrow(lat_ref, first, me * ROWS + first, EARLY)
    drain(early, early_send)
    drain(early, early_recv)
    for link in range(4):
        for which in range(2):
            p = PARTNER[link] if which else link
            narrow(early.at[link, which], 0, beside(link, -1) * ROWS + p * QUARTER, EARLY)

    starts(2, 4)

    @pl.when(me == 0)
    def _():
        pl.semaphore_wait(group_sem, NW - 1)
        for d in range(1, NZERO):
            pl.semaphore_signal(go_sem, inc=1, device_id=(d, wide), device_id_type=MESH)

    @pl.when(me != 0)
    def _():
        pl.semaphore_wait(go_sem, 1)

    nbuf[wide] = sums[:, :, COLS:]
    for d in range(1, NW):
        pltpu.make_async_remote_copy(
            src_ref=nbuf.at[wide], dst_ref=nbuf.at[wide], send_sem=na_send, recv_sem=na_recv,
            device_id=(me, lax.rem(wide + d, NW)), device_id_type=MESH,
        ).start()

    starts(4, 6)

    starts(6, 8)

    some = nbuf.at[pl.ds(0, NW - 1)]
    drain(some, na_send)
    drain(some, na_recv)
    lane = lax.broadcasted_iota(jnp.int32, (1, 128), 1)
    for r in range(NZERO * NW * NORM // 128):
        row = jnp.zeros((1, 128), jnp.float32)
        for d in range(128 * r // NORM, (128 * r + 127) // NORM + 1):
            shift = d * NORM - 128 * r
            moved = pltpu.roll(nbuf[d % NW, d // NW], shift % 128, 1)
            row = jnp.where((lane >= shift) & (lane < shift + NORM), moved, row)
        norm_ref[pl.ds(r, 1), :] = row

    starts(8, len(ORDER))

    drain(all_ref.at[pl.ds(0, 4 * sum(map(count, ORDER)))], send_sem)
    drain(all_ref.at[pl.ds(0, 4 * QUARTER * (len(ORDER) - len(GROUP)))], last_sem)


def write_kernel(
    all_ref, lat_ref, sq_ref, sk_ref, sv_ref, norm_ref,
    rq, rk, rv, cq, ck, cv, norm_out, lq, lk, lv,
    norm_buf, sem,
):
    copies = []
    for src, outs in ((all_ref, (rq, rk, rv)), (lat_ref, (lq, lk, lv))):
        first = 0
        for out in outs:
            width = out.shape[1]
            copies.append((src.at[:, pl.ds(first, width)], out))
            first += width
    copies += [(sq_ref, cq), (sk_ref, ck), (sv_ref, cv)]
    started = []
    for i, (src, dst) in enumerate(copies):
        copy = pltpu.make_async_copy(src, dst, sem.at[i])
        copy.start()
        started.append(copy)
    norm_buf[...] = norm_ref[...].astype(jnp.bfloat16)
    copy = pltpu.make_async_copy(norm_buf, norm_out, sem.at[len(copies)])
    copy.start()
    for done in started:
        done.wait()
    copy.wait()


def body(tq, sq, tk, sk, tv, sv, nt, ns):
    f32, bf16 = jnp.float32, jnp.bfloat16
    anyspace = pl.BlockSpec(memory_space=pl.ANY)
    hbm = pl.BlockSpec(memory_space=pltpu.HBM)
    dma = pltpu.SemaphoreType.DMA
    norm_rows = NZERO * NW * NORM // 128
    gathered = pl.pallas_call(
        gather_kernel,
        name="gather",
        out_shape=(
            jax.ShapeDtypeStruct((NZERO * ROWS, COLS), bf16),
            jax.ShapeDtypeStruct((ROWS, COLS), f32),
            jax.ShapeDtypeStruct((WQ // 128, 128), f32),
            jax.ShapeDtypeStruct((1, WK), f32),
            jax.ShapeDtypeStruct((1, WK), f32),
            jax.ShapeDtypeStruct((norm_rows, 128), f32),
        ),
        in_specs=[hbm] * 8,
        out_specs=(pl.BlockSpec(memory_space=pltpu.VMEM),) * 6,
        scratch_shapes=[
            pltpu.VMEM((2, ROWS, COLS), f32),
            pltpu.VMEM((NZERO, 1, COLS + 128), f32),
            pltpu.VMEM((NORM,), f32),
            pltpu.VMEM((NORM,), f32),
            pltpu.VMEM((NW, NZERO, 1, 128), f32),
            pltpu.VMEM((4, 2, EARLY, COLS), f32),
            dma((4,)),
            dma((2,)),
            dma, dma,
            dma, dma,
            dma, dma((len(GROUPS),)), dma,
            dma, dma,
            pltpu.SemaphoreType.REGULAR, pltpu.SemaphoreType.REGULAR,
        ],
        compiler_params=pltpu.CompilerParams(
            collective_id=0, has_side_effects=True, vmem_limit_bytes=26 * 2**20
        ),
    )(*(pltpu.with_memory_space_constraint(v, pltpu.HBM) for v in (tq, sq, tk, sk, tv, sv, nt, ns)))
    whole = NZERO * ROWS
    outs = pl.pallas_call(
        write_kernel,
        name="write",
        out_shape=(
            jax.ShapeDtypeStruct((whole, WQ), bf16),
            jax.ShapeDtypeStruct((whole, WK), bf16),
            jax.ShapeDtypeStruct((whole, WK), bf16),
            jax.ShapeDtypeStruct((WQ // 128, 128), f32),
            jax.ShapeDtypeStruct((1, WK), f32),
            jax.ShapeDtypeStruct((1, WK), f32),
            jax.ShapeDtypeStruct((norm_rows, 128), bf16),
            jax.ShapeDtypeStruct((ROWS, WQ), f32),
            jax.ShapeDtypeStruct((ROWS, WK), f32),
            jax.ShapeDtypeStruct((ROWS, WK), f32),
        ),
        in_specs=[anyspace] * 5 + [pl.BlockSpec(memory_space=pltpu.VMEM)],
        out_specs=(hbm,) * 10,
        scratch_shapes=[pltpu.VMEM((norm_rows, 128), bf16), dma((10,))],
        compiler_params=pltpu.CompilerParams(vmem_limit_bytes=2 * 2**20),
    )(*gathered)
    rq, rk, rv, cq, ck, cv, norm, lq, lk, lv = outs
    return (
        rq, rk, rv, cq.reshape(-1), ck.reshape(-1), cv.reshape(-1), norm.reshape(-1), lq, lk, lv
    )


def solution(mesh):
    both = P("zero", "width")
    in_specs = (both,) * 6 + (P(("zero", "width")),) * 2
    out_specs = (
        (P(None, "width"),) * 3 + (P("width"),) * 3 + (P(),) + (both,) * 3
    )
    return jax.shard_map(body, mesh=mesh, in_specs=in_specs, out_specs=out_specs, check_vma=False)
```

```python
import functools

import jax
import jax.numpy as jnp
from jax import lax
from jax.experimental import pallas as pl
from jax.experimental.pallas import tpu as pltpu
from jax.sharding import PartitionSpec as P

keep_rate = 0.5
MESH = pl.DeviceIdType.MESH

NZ, NY, NW = 4, 4, 8
NZERO = NZ * NY
ROWS = 448
WQ, WK = 896, 128
COLS = WQ + 2 * WK
QUARTER = ROWS // 4
SLAB = 16
EARLY = 16
NORM = 56

ORDER = (
    ("one", 0),
    ("two", 0, 0),
    ("one", 1),
    ("two", 1, 0),
    ("one", 2),
    ("two", 2, 0),
    ("two", 0, 1),
    ("two", 3, 0),
    ("two", 1, 1),
    ("two", 2, 1),
    ("two", 0, 2),
    ("two", 3, 1),
    ("two", 1, 2),
    ("two", 2, 2),
    ("two", 3, 2),
)
GROUPS = (
    (2, (("one", 0),)),
    (4, (("one", 1),)),
    (6, (("two", 0, 0), ("one", 2))),
    (8, (("two", 1, 0), ("two", 2, 0))),
    (10, (("two", 0, 1), ("two", 3, 0))),
    (12, (("two", 1, 1), ("two", 2, 1))),
    (14, (("two", 3, 1),)),
)
GROUP = {entry: g for g, (_, entries) in enumerate(GROUPS) for entry in entries}
FIRST = (("one", 0), ("two", 0, 0))
OTHERS = sorted(
    ((dz, dy) for dz in range(NZ) for dy in range(NY) if dz or dy),
    key=lambda d: -min(d[0], NZ - d[0]) - min(d[1], NY - d[1]),
)
LINKS = (("y", 1), ("y", -1), ("z", 1), ("z", -1))
PARTNER = (2, 3, 0, 1)


def gather_kernel(
    tq, sq, tk, sk, tv, sv, nt, ns,
    all_ref, lat_ref, cq_ref, ck_ref, cv_ref, norm_ref,
    inbuf, sums, ntb, nsb, nbuf, early,
    load_sem, nload_sem, sum_send, sum_recv, na_send, na_recv,
    send_sem, recv_sem, last_sem, early_send, early_recv, group_sem, go_sem,
):
    me = lax.axis_index("zero")
    wide = lax.axis_index("width")
    z, y = me // NY, me % NY

    def at(zz, yy):
        return lax.rem(zz + 2 * NZ, NZ) * NY + lax.rem(yy + 2 * NY, NY)

    def drain(ref, sem):
        pltpu.make_async_copy(ref, ref, sem).wait()

    barrier = pltpu.get_barrier_semaphore()
    for dz, dy in OTHERS:
        pl.semaphore_signal(
            barrier, inc=1, device_id=(at(z + dz, y + dy), wide), device_id_type=MESH
        )

    @pl.when(me == 0)
    def _():
        for d in range(1, NW):
            pl.semaphore_signal(
                barrier, inc=1, device_id=(me, lax.rem(wide + d, NW)), device_id_type=MESH
            )

    for c in range(2):
        rows = pl.ds(c * 2 * QUARTER, 2 * QUARTER)
        for i, (src, first, width) in enumerate((
            (tq, 0, WQ), (sq, 0, WQ), (tk, WQ, WK), (sk, WQ, WK), (tv, WQ + WK, WK), (sv, WQ + WK, WK)
        )):
            pltpu.make_async_copy(
                src.at[rows], inbuf.at[i % 2, rows, pl.ds(first, width)], load_sem.at[c]
            ).start()
    nload = (
        pltpu.make_async_copy(nt, ntb, nload_sem.at[0]),
        pltpu.make_async_copy(ns, nsb, nload_sem.at[1]),
    )
    for copy in nload:
        copy.start()

    acc = jnp.zeros((8, COLS), jnp.float32)
    for c in range(2):
        drain(inbuf.at[:, pl.ds(c * 2 * QUARTER, 2 * QUARTER)], load_sem.at[c])

        def average(i, acc):
            rows = pl.ds(pl.multiple_of(c * 2 * QUARTER + i * SLAB, SLAB), SLAB)
            latest = keep_rate * inbuf[1, rows, :] + (1.0 - keep_rate) * inbuf[0, rows, :]
            lat_ref[rows, :] = latest
            square = latest * latest
            return acc + square[:8] + square[8:]

        acc = lax.fori_loop(0, 2 * QUARTER // SLAB, average, acc, unroll=7)
    for copy in nload:
        copy.wait()
    gain = (ntb[...] + nsb[...]).reshape(1, NORM)
    sums[me] = jnp.concatenate(
        [jnp.sum(acc, axis=0, keepdims=True), gain, jnp.zeros((1, 128 - NORM), jnp.float32)], axis=1
    )

    @pl.when(me == 0)
    def _():
        pl.semaphore_wait(barrier, NZERO - 1 + NW - 1)

    @pl.when(me != 0)
    def _():
        pl.semaphore_wait(barrier, NZERO - 1)

    for dz, dy in OTHERS:
        pltpu.make_async_remote_copy(
            src_ref=sums.at[me], dst_ref=sums.at[me], send_sem=sum_send, recv_sem=sum_recv,
            device_id=(at(z + dz, y + dy), wide), device_id_type=MESH,
        ).start()

    def beside(link, steps):
        ring, sign = LINKS[link]
        return at(z + sign * steps, y) if ring == "z" else at(z, y + sign * steps)

    for which in range(2):
        for link in range(4):
            p = PARTNER[link] if which else link
            pltpu.make_async_remote_copy(
                src_ref=lat_ref.at[pl.ds(p * QUARTER, EARLY)], dst_ref=early.at[link, which],
                send_sem=early_send, recv_sem=early_recv,
                device_id=(beside(link, 1), wide), device_id_type=MESH,
            ).start()

    @pl.when(me == 0)
    def _():
        for d in range(1, NW):
            pl.semaphore_signal(
                group_sem, inc=1, device_id=(me, lax.rem(wide + d, NW)), device_id_type=MESH
            )

    some = sums.at[pl.ds(0, NZERO - 1)]
    drain(some, sum_send)
    drain(some, sum_recv)

    total = sums[0, :, :COLS]
    for d in range(1, NZERO):
        total = total + sums[d, :, :COLS]
    scale = jnp.sqrt(total)
    inverse = jnp.broadcast_to(1.0 / scale, (SLAB, COLS))

    def piece(p, zz, yy, skip):
        first = at(zz, yy) * ROWS + p * QUARTER + skip
        return pl.ds(pl.multiple_of(first, 8), QUARTER - skip)

    def count(entry):
        return QUARTER - EARLY if entry in FIRST else QUARTER

    def start(link, slot):
        ring, sign = LINKS[link]
        entry = ORDER[slot]
        if entry[0] == "one":
            p, steps = link, {ring: entry[1]}
        else:
            p = PARTNER[link]
            steps = {ring: entry[2], LINKS[p][0]: entry[1]}
        skip = QUARTER - count(entry)
        rows = piece(p, z - sign * steps.get("z", 0), y - sign * steps.get("y", 0), skip)
        arrived = recv_sem.at[GROUP[entry]] if entry in GROUP else last_sem
        pltpu.make_async_remote_copy(
            src_ref=all_ref.at[rows], dst_ref=all_ref.at[rows], send_sem=send_sem, recv_sem=arrived,
            device_id=(beside(link, 1), wide), device_id_type=MESH,
        ).start()

    def starts(first, last):
        for slot in range(first, last):
            for g, (when, entries) in enumerate(GROUPS):
                if when == slot:
                    drain(all_ref.at[pl.ds(0, 4 * sum(map(count, entries)))], recv_sem.at[g])
            for link in range(4):
                start(link, slot)

    def narrow(src, first, there, count):
        def some(at_row, height):
            rows = pl.ds(pl.multiple_of(first + at_row, 8), height)
            out = pl.ds(pl.multiple_of(there + at_row, 8), height)
            all_ref[out, :] = (src[rows, :] * inverse[:height]).astype(jnp.bfloat16)

        def step(i, _):
            some(i * SLAB, SLAB)
            return 0

        lax.fori_loop(0, count // SLAB, step, 0, unroll=True)
        if count % SLAB:
            some(count // SLAB * SLAB, count % SLAB)

    for p in range(4):
        first = p * QUARTER + EARLY
        narrow(lat_ref, first, me * ROWS + first, QUARTER - EARLY)
        start(p, 0)
        if p >= 2:
            start(p, 1)
    for link in range(2):
        start(link, 1)
    for r in range(WQ // 128):
        cq_ref[pl.ds(r, 1), :] = scale[:, r * 128 : (r + 1) * 128]
    ck_ref[...] = scale[:, WQ : WQ + WK]
    cv_ref[...] = scale[:, WQ + WK :]
    for p in range(4):
        first = p * QUARTER
        narrow(lat_ref, first, me * ROWS + first, EARLY)
    drain(early, early_send)
    drain(early, early_recv)
    for link in range(4):
        for which in range(2):
            p = PARTNER[link] if which else link
            narrow(early.at[link, which], 0, beside(link, -1) * ROWS + p * QUARTER, EARLY)

    starts(2, 4)

    @pl.when(me == 0)
    def _():
        pl.semaphore_wait(group_sem, NW - 1)
        for d in range(1, NZERO):
            pl.semaphore_signal(go_sem, inc=1, device_id=(d, wide), device_id_type=MESH)

    @pl.when(me != 0)
    def _():
        pl.semaphore_wait(go_sem, 1)

    nbuf[wide] = sums[:, :, COLS:]
    for d in range(1, NW):
        pltpu.make_async_remote_copy(
            src_ref=nbuf.at[wide], dst_ref=nbuf.at[wide], send_sem=na_send, recv_sem=na_recv,
            device_id=(me, lax.rem(wide + d, NW)), device_id_type=MESH,
        ).start()

    starts(4, 6)

    starts(6, 8)

    some = nbuf.at[pl.ds(0, NW - 1)]
    drain(some, na_send)
    drain(some, na_recv)
    lane = lax.broadcasted_iota(jnp.int32, (1, 128), 1)
    for r in range(NZERO * NW * NORM // 128):
        row = jnp.zeros((1, 128), jnp.float32)
        for d in range(128 * r // NORM, (128 * r + 127) // NORM + 1):
            shift = d * NORM - 128 * r
            moved = pltpu.roll(nbuf[d % NW, d // NW], shift % 128, 1)
            row = jnp.where((lane >= shift) & (lane < shift + NORM), moved, row)
        norm_ref[pl.ds(r, 1), :] = row

    starts(8, len(ORDER))

    drain(all_ref.at[pl.ds(0, 4 * sum(map(count, ORDER)))], send_sem)
    drain(all_ref.at[pl.ds(0, 4 * QUARTER * (len(ORDER) - len(GROUP)))], last_sem)


def write_kernel(
    all_ref, lat_ref, sq_ref, sk_ref, sv_ref, norm_ref,
    rq, rk, rv, cq, ck, cv, norm_out, lq, lk, lv,
    norm_buf, sem,
):
    copies = []
    for src, outs in ((all_ref, (rq, rk, rv)), (lat_ref, (lq, lk, lv))):
        first = 0
        for out in outs:
            width = out.shape[1]
            copies.append((src.at[:, pl.ds(first, width)], out))
            first += width
    copies += [(sq_ref, cq), (sk_ref, ck), (sv_ref, cv)]
    started = []
    for i, (src, dst) in enumerate(copies):
        copy = pltpu.make_async_copy(src, dst, sem.at[i])
        copy.start()
        started.append(copy)
    norm_buf[...] = norm_ref[...].astype(jnp.bfloat16)
    copy = pltpu.make_async_copy(norm_buf, norm_out, sem.at[len(copies)])
    copy.start()
    for done in started:
        done.wait()
    copy.wait()


def body(tq, sq, tk, sk, tv, sv, nt, ns):
    f32, bf16 = jnp.float32, jnp.bfloat16
    anyspace = pl.BlockSpec(memory_space=pl.ANY)
    hbm = pl.BlockSpec(memory_space=pltpu.HBM)
    dma = pltpu.SemaphoreType.DMA
    norm_rows = NZERO * NW * NORM // 128
    gathered = pl.pallas_call(
        gather_kernel,
        name="gather",
        out_shape=(
            jax.ShapeDtypeStruct((NZERO * ROWS, COLS), bf16),
            jax.ShapeDtypeStruct((ROWS, COLS), f32),
            jax.ShapeDtypeStruct((WQ // 128, 128), f32),
            jax.ShapeDtypeStruct((1, WK), f32),
            jax.ShapeDtypeStruct((1, WK), f32),
            jax.ShapeDtypeStruct((norm_rows, 128), f32),
        ),
        in_specs=[hbm] * 8,
        out_specs=(pl.BlockSpec(memory_space=pltpu.VMEM),) * 6,
        scratch_shapes=[
            pltpu.VMEM((2, ROWS, COLS), f32),
            pltpu.VMEM((NZERO, 1, COLS + 128), f32),
            pltpu.VMEM((NORM,), f32),
            pltpu.VMEM((NORM,), f32),
            pltpu.VMEM((NW, NZERO, 1, 128), f32),
            pltpu.VMEM((4, 2, EARLY, COLS), f32),
            dma((4,)),
            dma((2,)),
            dma, dma,
            dma, dma,
            dma, dma((len(GROUPS),)), dma,
            dma, dma,
            pltpu.SemaphoreType.REGULAR, pltpu.SemaphoreType.REGULAR,
        ],
        compiler_params=pltpu.CompilerParams(
            collective_id=0, has_side_effects=True, vmem_limit_bytes=26 * 2**20
        ),
    )(*(pltpu.with_memory_space_constraint(v, pltpu.HBM) for v in (tq, sq, tk, sk, tv, sv, nt, ns)))
    whole = NZERO * ROWS
    outs = pl.pallas_call(
        write_kernel,
        name="write",
        out_shape=(
            jax.ShapeDtypeStruct((whole, WQ), bf16),
            jax.ShapeDtypeStruct((whole, WK), bf16),
            jax.ShapeDtypeStruct((whole, WK), bf16),
            jax.ShapeDtypeStruct((WQ // 128, 128), f32),
            jax.ShapeDtypeStruct((1, WK), f32),
            jax.ShapeDtypeStruct((1, WK), f32),
            jax.ShapeDtypeStruct((norm_rows, 128), bf16),
            jax.ShapeDtypeStruct((ROWS, WQ), f32),
            jax.ShapeDtypeStruct((ROWS, WK), f32),
            jax.ShapeDtypeStruct((ROWS, WK), f32),
        ),
        in_specs=[anyspace] * 5 + [pl.BlockSpec(memory_space=pltpu.VMEM)],
        out_specs=(hbm,) * 10,
        scratch_shapes=[pltpu.VMEM((norm_rows, 128), bf16), dma((10,))],
        compiler_params=pltpu.CompilerParams(vmem_limit_bytes=2 * 2**20),
    )(*gathered)
    rq, rk, rv, cq, ck, cv, norm, lq, lk, lv = outs
    return (
        rq, rk, rv, cq.reshape(-1), ck.reshape(-1), cv.reshape(-1), norm.reshape(-1), lq, lk, lv
    )


def solution(mesh):
    both = P("zero", "width")
    in_specs = (both,) * 6 + (P(("zero", "width")),) * 2
    out_specs = (
        (P(None, "width"),) * 3 + (P("width"),) * 3 + (P(),) + (both,) * 3
    )
    return jax.shard_map(body, mesh=mesh, in_specs=in_specs, out_specs=out_specs, check_vma=False)
```
